32 devices in a mesh: tok: 8 (over z, core), col: 4 (over y, x).
Axes of the slice: x: 2, y: 2, z: 4, core: 2. Of those that a mesh axis runs over, the one named last changes fastest.
Arguments:
- tokens: bfloat16 [8192, 4096], P('tok'), may hold values from -6 to 6
- grads_out: bfloat16 [8192, 8192], P('tok', 'col'), may hold values from -0.0625 to 0.0625
- statistics: float32 [8, 8, 1024, 1024], P('col', 'tok'), as said below
Outputs:
- update: bfloat16 [4096, 8192], P('tok', 'col')
- new_statistics: float32 [8, 8, 1024, 1024], P('col', 'tok')
The draws below stay inside these ranges and needn't reach their ends.
Inputs may be any that keep to these rules, and one draw needn't show every extreme that they name: statistics[j, (2 i + s) + w] holds columns w * 1024 onward of a symmetric positive definite matrix with a positive diagonal.
All inputs are finite; a program needn't handle non-finite values.
Results may differ from the reference program's by a relative error of at most 0.007.
Values may be sent and summed in bfloat16 or wider, within the bound.
A program may use at most 128 MiB of HBM per device.

```python
import math
import jax
import jax.numpy as jnp
from jax import lax

D = 4096
QUERY = 8192
ORDER = 1024
ITERS = 3
TOKENS = 8192
ROW_BLOCKS = 4
COL_BLOCKS = 8
PIECES = 1
N_TOK = 8


def draw_statistics(key, part):
    number_mats = COL_BLOCKS * ROW_BLOCKS * 2

    def one_matrix(seed_key):
        key_base, key_diag = jax.random.split(seed_key)
        base = jax.random.normal(key_base, (ORDER, ORDER), jnp.float32)
        rank_index = jnp.arange(1, ORDER + 1, dtype=jnp.float32)
        exponent = 1.0
        diagonal = jnp.exp(jax.random.uniform(key_diag, (ORDER,), jnp.float32, math.log(0.25 * ORDER), math.log(2.0 * ORDER)))
        strengths = 64.0 * ORDER * jnp.power(rank_index, -exponent)
        weighted = base * strengths[None, :]
        return jnp.dot(weighted, base.T, precision=lax.Precision.HIGHEST) / ORDER + jnp.diag(diagonal)
    matrices = lax.map(one_matrix, jax.random.split(jax.random.fold_in(key, 17), number_mats))
    matrices = matrices.reshape(COL_BLOCKS, ROW_BLOCKS, 2, ORDER, PIECES, ORDER // PIECES)
    return jnp.transpose(matrices, (0, 1, 2, 4, 3, 5)).reshape(COL_BLOCKS, 2 * ROW_BLOCKS * PIECES, ORDER, ORDER // PIECES)


def levels(rng, extent, cuts, smallest, high):
    def one(axis_at, shards_of):
        draws = jax.random.uniform(jax.random.fold_in(jax.random.fold_in(rng, 6), axis_at), (shards_of,), jnp.float32, smallest / len(cuts), high / len(cuts))
        return jnp.repeat(jnp.exp(draws), extent[axis_at] // shards_of).reshape((-1,) + (1,) * (len(extent) - axis_at - 1))

    factor_of = one(*cuts[0])
    for cut in cuts[1:]:
        factor_of = factor_of * one(*cut)
    return factor_of


def centred(own_key, shape, width, limit, cuts=(), kind=jnp.bfloat16):
    level = levels(own_key, shape, cuts, -0.22, 0.18) if cuts else 1.0
    array = jax.random.normal(own_key, shape, jnp.float32) * width * level
    return jnp.minimum(jnp.maximum(array, -limit), limit).astype(kind)


def setup_inputs(seed: int = 0) -> dict:
    splits = jax.random.split(jax.random.key(seed), 4)
    return {
        "tokens": centred(splits[0], (TOKENS, D), 1.0, 6.0, ((0, 8),)),
        "grads_out": centred(splits[1], (TOKENS, QUERY), TOKENS ** -0.5, 0.0625, ((0, 8), (1, 4))),
        "statistics": draw_statistics(jax.random.fold_in(splits[3], 71), 0),
    }


def inverse_root(statistic):
    identity = jnp.eye(statistic.shape[0], dtype=jnp.float32)
    scaling = 2.5 / jnp.sqrt(jnp.sum(statistic * statistic) + 1e-06)
    matrix = scaling * statistic
    factor = (5.0 * identity - matrix) * 0.25
    iterate = jnp.sqrt(jnp.sqrt(scaling)) * factor
    for repeat in range(1, ITERS):
        square = jnp.dot(factor, factor, precision=lax.Precision.HIGHEST)
        fourth = jnp.dot(square, square, precision=lax.Precision.HIGHEST)
        matrix = jnp.dot(fourth, matrix, precision=lax.Precision.HIGHEST)
        factor = (5.0 * identity - matrix) * 0.25
        iterate = jnp.dot(factor, iterate, precision=lax.Precision.HIGHEST)
    return iterate

def reference(tokens, grads_out, statistics):
    pieces = N_TOK // (2 * ROW_BLOCKS)
    assembled = statistics.reshape(COL_BLOCKS, ROW_BLOCKS, 2, pieces, ORDER, ORDER // pieces)
    assembled = jnp.transpose(assembled, (0, 1, 2, 4, 3, 5)).reshape(COL_BLOCKS, ROW_BLOCKS, 2, ORDER, ORDER)
    scale_factor = math.sqrt(ORDER)

    def one_column(column_index):
        columns = lax.dynamic_slice_in_dim(grads_out, column_index * ORDER, ORDER, 1)
        gradient = lax.dot_general(tokens, columns, (((0,), (0,)), ((), ())), preferred_element_type=jnp.float32)
        grad_blocks = gradient.astype(jnp.bfloat16).reshape(ROW_BLOCKS, ORDER, ORDER)
        previous = lax.dynamic_index_in_dim(assembled, column_index, 0, keepdims=False)

        def one_block(inputs_pair):
            grad_block, old_stats = inputs_pair
            left_stat = old_stats[0] + jnp.dot(grad_block, grad_block.T, preferred_element_type=jnp.float32)
            right_stat = old_stats[1] + jnp.dot(grad_block.T, grad_block, preferred_element_type=jnp.float32)
            left_root = inverse_root(left_stat).astype(jnp.bfloat16)
            right_root = inverse_root(right_stat).astype(jnp.bfloat16)
            mixed_rows = jnp.dot(left_root, grad_block, preferred_element_type=jnp.float32).astype(jnp.bfloat16)
            update = (jnp.dot(mixed_rows, right_root, preferred_element_type=jnp.float32) * scale_factor).astype(jnp.bfloat16)
            return (update, jnp.stack([left_stat, right_stat]))
        return lax.map(one_block, (grad_blocks, previous))
    updates, fresh_stats = lax.map(one_column, jnp.arange(COL_BLOCKS, dtype=jnp.int32))
    update = jnp.transpose(updates, (1, 2, 0, 3)).reshape(ROW_BLOCKS * ORDER, COL_BLOCKS * ORDER)
    fresh_stats = fresh_stats.reshape(COL_BLOCKS, ROW_BLOCKS, 2, ORDER, pieces, ORDER // pieces)
    fresh_stats = jnp.transpose(fresh_stats, (0, 1, 2, 4, 3, 5)).reshape(COL_BLOCKS, ROW_BLOCKS * 2 * pieces, ORDER, ORDER // pieces)
    return (update, fresh_stats)
```

```python
import functools
import math

import jax
import jax.numpy as jnp
from jax import lax
from jax.experimental import pallas as pl
from jax.experimental.pallas import tpu as pltpu
from jax.sharding import PartitionSpec as P

ITERS = 3


def swapped(block, axis, bit):
    count = lax.axis_size(axis)
    route = []
    for low in range(count):
        high = low | 1 << bit
        if high != low and high < count:
            route += [(low, high), (high, low)]
    return lax.ppermute(block, axis, route)


def as_sent(array):
    return jax.tree.map(lambda a: a.astype(jnp.bfloat16) if a.dtype == jnp.float32 else a, array)


def doubling(values, levels, device, axis_dim, partner):
    for level_bit in range(levels):
        partner_part = partner(values, level_bit)
        low_side = device // 2**level_bit % 2 == 0
        values = jnp.where(
            low_side,
            jnp.concatenate([values, partner_part], axis_dim),
            jnp.concatenate([partner_part, values], axis_dim),
        )
    return values


def product(left_side, right_side):
    return jnp.einsum("bij,bjk->bik", left_side, right_side, precision=lax.Precision.HIGHEST)


def in_pieces(tokens, grads_out, statistics):
    device = lax.axis_index("tok")
    blocks = statistics.shape[0]
    order_size = statistics.shape[2]
    piece_width = statistics.shape[3]
    pieces = order_size // piece_width
    levels = pieces.bit_length() - 1
    rows_dev = tokens.shape[1] // lax.axis_size("tok")
    side_bit = device // pieces % 2
    column = device % pieces
    slab_index = device % (2 * pieces)

    def columns_of(values):
        return lax.dynamic_slice_in_dim(values, column * piece_width, piece_width, 2)

    owned = lax.psum_scatter(
        lax.dot_general(
            tokens, grads_out, (((0,), (0,)), ((), ())), preferred_element_type=jnp.float32
        ),
        "tok",
        scatter_dimension=0,
        tiled=True,
    ).astype(jnp.bfloat16)
    gradient = doubling(
        owned, levels + 1, device, 0, lambda portion, level_bit: swapped(portion, "tok", level_bit)
    )
    grad_cube = gradient.reshape(order_size, blocks, order_size)
    forward = jnp.transpose(grad_cube, (1, 0, 2))
    backward = jnp.transpose(grad_cube, (1, 2, 0))
    oriented = jnp.where(side_bit == 0, forward, backward)
    own_rows = lax.dynamic_slice_in_dim(oriented, column * piece_width, piece_width, 1)
    gram_piece = jnp.einsum("brc,bqc->brq", oriented, own_rows, preferred_element_type=jnp.float32)
    fresh_stat = statistics[:, 0] + gram_piece
    identity = jnp.eye(order_size, dtype=jnp.float32)

    def widen(values):
        return doubling(
            values, levels, device, 2, lambda portion, level_bit: swapped(portion, "tok", level_bit)
        )

    assembled = widen(fresh_stat)
    scaling = (2.5 / jnp.sqrt(jnp.sum(assembled * assembled, axis=(1, 2)) + 1e-06))[:, None, None]
    matrix = scaling * assembled
    factor = (5.0 * identity - matrix) * 0.25
    iterate = jnp.sqrt(jnp.sqrt(scaling)) * columns_of(factor)
    for repeat in range(1, ITERS):
        square = widen(product(factor, columns_of(factor)))
        fourth = widen(product(square, columns_of(square)))
        matrix = widen(product(fourth, columns_of(matrix)))
        factor = (5.0 * identity - matrix) * 0.25
        iterate = product(factor, iterate)
    own_root = doubling(
        iterate.astype(jnp.bfloat16),
        levels,
        device,
        2,
        lambda portion, level_bit: jax.tree.map(
            lambda part, own: part.astype(own.dtype),
            swapped(as_sent(portion), "tok", level_bit),
            portion,
        ),
    )
    other_root = swapped(own_root, "tok", levels)
    left_root = jnp.where(side_bit == 0, own_root, other_root)
    right_root = jnp.where(side_bit == 0, other_root, own_root)
    left_rows = lax.dynamic_slice_in_dim(left_root, slab_index * rows_dev, rows_dev, 1)
    mixed_rows = jnp.einsum(
        "bsr,rbc->bsc", left_rows, grad_cube, preferred_element_type=jnp.float32
    ).astype(jnp.bfloat16)
    update = jnp.einsum(
        "bsc,bcd->sbd", mixed_rows, right_root, preferred_element_type=jnp.float32
    ) * math.sqrt(order_size)
    return (update.reshape(rows_dev, blocks * order_size).astype(jnp.bfloat16), fresh_stat[:, None])


LINE = 4
SENDS = 3
SLOTS = 5


def fused_kernel(
    blocks, tokens, grads, old, update, fresh,
    tok2, grad2, sent, got, own32, grad, stat, scaled, one, two, three, rest, roots, mixed, staged,
    tok_in, tok_send, tok_recv, grad_in, grad_send, grad_recv, hop_send, hop_recv,
    half_send, half_recv, stat_in, stat_out, root_send, root_recv, update_out,
):
    f32, bf16 = jnp.float32, jnp.bfloat16
    order = grad.shape[1]
    local = tokens.shape[0]
    rows = order // 2
    wide = order // 2
    tile = order // 4
    me = lax.axis_index("tok")
    spot, core = me // 2, lax.rem(me, 2)
    partner = spot * 2 + 1 - core
    outer = jnp.logical_or(spot == 0, spot == LINE - 1)
    inner = jnp.logical_not(outer)
    low = spot < LINE // 2
    near = spot + 1 - 2 * lax.rem(spot, 2)
    across = LINE - 1 - spot
    near_device, across_device = near * 2 + core, across * 2 + core

    def chunk_of(k):
        far = jnp.where(low, LINE - 1 - k, k)
        return jnp.where(k < 2, far, jnp.where(k == 2, near, spot))

    def remote(source, target, send, recv, device):
        return pltpu.make_async_remote_copy(
            src_ref=source, dst_ref=target, send_sem=send, recv_sem=recv,
            device_id={"tok": device}, device_id_type=pl.DeviceIdType.MESH,
        )

    def columns(k, owner):
        return pl.ds(pl.multiple_of((chunk_of(k) * 2 + owner) * rows, rows), rows)

    def tok_local(k):
        return pltpu.make_async_copy(
            tokens.at[:, columns(k, core)], tok2.at[k, pl.ds(0, local), :], tok_in.at[k]
        )

    def tok_remote(k):
        return remote(
            tokens.at[:, columns(k, 1 - core)], tok2.at[k, pl.ds(local, local), :],
            tok_send.at[k], tok_recv.at[k], partner,
        )

    def grad_columns(j, h):
        return pl.ds(pl.multiple_of(j * order + h * wide, wide), wide)

    def grad_local(j, h):
        return pltpu.make_async_copy(
            grads.at[:, grad_columns(j, h)], grad2.at[j, h, pl.ds(0, local), :], grad_in.at[j, h]
        )

    def grad_remote(j, h):
        return remote(
            grads.at[:, grad_columns(j, h)], grad2.at[j, h, pl.ds(local, local), :],
            grad_send.at[j, h], grad_recv.at[j, h], partner,
        )

    def stat_load(j):
        return pltpu.make_async_copy(old.at[j, 0], stat, stat_in.at[0])

    def stat_store(j):
        return pltpu.make_async_copy(stat, fresh.at[j, 0], stat_out.at[0])

    def hop(j, k, h):
        slot = jnp.where(jnp.logical_or(outer, k == 2), k, SENDS + k)
        device = jnp.where(jnp.logical_or(outer, k == 2), near_device, across_device)
        return remote(
            sent.at[j, k, h], got.at[j, slot, h], hop_send.at[j, k, h], hop_recv.at[j, slot, h],
            device,
        )

    def arrived(j, slot, h):
        remote(
            sent.at[j, 0, h], got.at[j, slot, h], hop_send.at[j, 0, h], hop_recv.at[j, slot, h],
            near_device,
        ).wait_recv()

    def half(j, h):
        part = grad.at[j, pl.ds(pl.multiple_of(core * rows, rows), rows), pl.ds(h * wide, wide)]
        return remote(part, part, half_send.at[j, h], half_recv.at[j, h], partner)

    def half_arrived(j, h):
        part = grad.at[
            j, pl.ds(pl.multiple_of((1 - core) * rows, rows), rows), pl.ds(h * wide, wide)
        ]
        remote(part, part, half_send.at[j, h], half_recv.at[j, h], partner).wait_recv()

    def root_piece(n, side):
        part = roots.at[side, pl.ds(n * tile, tile), :]
        return remote(part, part, root_send.at[n], root_recv.at[n], partner)

    def update_store(j):
        return pltpu.make_async_copy(
            staged, update.at[:, pl.ds(pl.multiple_of(j * order, order), order)], update_out.at[0]
        )

    barrier = pltpu.get_barrier_semaphore()
    pl.semaphore_signal(
        barrier, inc=1, device_id={"tok": partner}, device_id_type=pl.DeviceIdType.MESH
    )
    pl.semaphore_signal(
        barrier, inc=1, device_id={"tok": near_device}, device_id_type=pl.DeviceIdType.MESH
    )

    @pl.when(inner)
    def _():
        pl.semaphore_signal(
            barrier, inc=1, device_id={"tok": across_device}, device_id_type=pl.DeviceIdType.MESH
        )

    tok_local(0).start()
    grad_local(0, 0).start()
    pl.semaphore_wait(barrier, jnp.where(inner, 3, 2))
    tok_remote(0).start()
    grad_remote(0, 0).start()
    for h in range(2):
        if h:
            grad_local(0, h).start()
            grad_remote(0, h).start()
    for k in range(1, 4):
        tok_local(k).start()
        tok_remote(k).start()
    for j in range(1, blocks):
        for h in range(2):
            grad_local(j, h).start()
            grad_remote(j, h).start()
    stat_load(0).start()

    def wait_tokens(k):
        tok_local(k).wait()
        tok_remote(k).wait_recv()

    def wait_grads(j, h):
        grad_local(j, h).wait()
        grad_remote(j, h).wait_recv()

    def partial(j, k, h):
        return lax.dot_general(
            tok2[k], grad2[j, h], (((0,), (0,)), ((), ())), preferred_element_type=f32
        )

    def step(s, carry):
        j, k = s // SENDS, lax.rem(s, SENDS)

        @pl.when(j == 0)
        def _():
            wait_tokens(k)

        for h in range(2):

            @pl.when(k == 0)
            def _():
                wait_grads(j, h)

            sent_part = partial(j, k, h)

            @pl.when(outer)
            def _():
                sent[j, k, h] = sent_part.astype(bf16)

            @pl.when(inner)
            def _():
                slot = jnp.where(k == 2, SENDS, k)
                arrived(j, slot, h)
                sent[j, k, h] = (sent_part + got[j, slot, h].astype(f32)).astype(bf16)

            hop(j, k, h).start()
        return carry

    def put(ref, n, value):
        value = value.astype(bf16)
        ref[n : n + tile, n:] = value
        if n + tile < order:
            ref[n + tile :, n : n + tile] = value[:, tile:].T

    def product(left, right, finish):
        for n in range(0, order, tile):
            total = jnp.dot(left[n : n + tile, :], right[:, n:], preferred_element_type=f32)
            finish(total, n, (slice(n, n + tile), slice(n, None)))

    def one_block(j, carry):
        split = jnp.where(outer, blocks * SENDS, SENDS)
        lax.fori_loop(
            jnp.where(j == 0, 0, jnp.maximum(split, j * SENDS)),
            jnp.where(j == 0, split, jnp.maximum(split, (j + 1) * SENDS)),
            step,
            0,
        )

        @pl.when(j == 0)
        def _():
            wait_tokens(SENDS)

        for h in range(2):
            own32[h] = partial(j, SENDS, h)
        for h in range(2):
            arrived(j, 2, h)

            @pl.when(outer)
            def _():
                own32[h] = own32[h] + got[j, 2, h].astype(f32)

            @pl.when(inner)
            def _():
                arrived(j, SENDS + 1, h)
                own32[h] = (
                    own32[h] + got[j, 2, h].astype(f32) + got[j, SENDS + 1, h].astype(f32)
                )

            grad[j, pl.ds(pl.multiple_of(core * rows, rows), rows), h * wide : (h + 1) * wide] = (
                own32[h].astype(bf16)
            )
            half(j, h).start()
        stat_load(j).wait()
        for h in range(2):
            half_arrived(j, h)

        def gram(left):
            sums = jnp.zeros((1, order), f32)
            for n in range(0, order, tile):
                if left:
                    total = lax.dot_general(
                        grad[j, n : n + tile, :], grad[j, n:, :], (((1,), (1,)), ((), ())),
                        preferred_element_type=f32,
                    )
                else:
                    total = lax.dot_general(
                        grad[j, :, n : n + tile], grad[j, :, n:], (((0,), (0,)), ((), ())),
                        preferred_element_type=f32,
                    )
                total = total + stat[n : n + tile, n:]
                stat[n : n + tile, n:] = total
                square = jnp.sum(total * total, axis=0, keepdims=True)
                own = jnp.sum(square[:, :tile], axis=1, keepdims=True)
                if n + tile < order:
                    stat[n + tile :, n : n + tile] = total[:, tile:].T
                    own = own + 2.0 * jnp.sum(square[:, tile:], axis=1, keepdims=True)
                sums = sums + own
            own32[0, 0:1, :] = sums[:, :wide]

        pl.when(core == 0)(lambda: gram(True))
        pl.when(core == 1)(lambda: gram(False))
        stat_store(j).start()
        zeta = 2.5 / jnp.sqrt(own32[0, 0:1, 0:1] + 1e-06)
        gain = jnp.sqrt(jnp.sqrt(zeta))
        scaled[...] = (zeta * stat[...]).astype(bf16)

        def first_square(total, n, at):
            put(one, n, (total - 10.0 * scaled[at].astype(f32)) * 0.0625)

        product(scaled, scaled, first_square)

        def first_fourth(total, n, at):
            put(two, n, 3.125 * one[at].astype(f32) + total)

        product(one, one, first_fourth)

        def second(total, n, at):
            put(three, n, (2.44140625 * zeta) * stat[at] + total)

        product(two, scaled, second)

        def second_square(total, n, at):
            base = three[at].astype(f32)
            put(one, n, (total - 10.0 * base) * 0.0625)
            put(two, n, (5.0 * base - total) * 0.25)

        product(three, three, second_square)
        mine = roots.at[core]

        def second_fourth(total, n, at):
            put(mine, n, 3.125 * one[at].astype(f32) + total)

        product(one, one, second_fourth)

        def factors(total, n, at):
            value = -0.25 * (
                1.25 * three[at].astype(f32) + 2.44140625 * two[at].astype(f32) + total
            )
            rest[at] = value
            put(one, n, value)

        product(mine, two, factors)

        def final(total, n, at):
            shape = total.shape
            unit = (
                lax.broadcasted_iota(jnp.int32, shape, 0)
                == lax.broadcasted_iota(jnp.int32, shape, 1)
            ).astype(f32)
            value = (
                1.953125 * unit + 1.25 * rest[at] - (0.390625 * zeta) * stat[at] - 0.25 * total
            )
            put(mine, n, gain * value)
            root_piece(n // tile, core).start()

        product(one, scaled, final)

        def roots_arrived():
            for n in range(4):
                root_piece(n, 1 - core).wait_recv()

        pl.when(core == 1)(roots_arrived)
        left = roots[0, pl.ds(pl.multiple_of(core * rows, rows), rows), :]
        mixed[...] = jnp.dot(left, grad[j], preferred_element_type=f32).astype(bf16)
        pl.when(core == 0)(roots_arrived)

        @pl.when(j > 0)
        def _():
            update_store(j - 1).wait()

        staged[...] = (
            jnp.dot(mixed[...], roots[1], preferred_element_type=f32) * math.sqrt(order)
        ).astype(bf16)
        update_store(j).start()
        for n in range(4):
            root_piece(n, core).wait_send()
        stat_store(j).wait()

        @pl.when(j < blocks - 1)
        def _():
            stat_load(j + 1).start()

        return carry

    lax.fori_loop(0, blocks, one_block, 0)
    update_store(blocks - 1).wait()
    for k in range(4):
        tok_remote(k).wait_send()
    for j in range(blocks):
        for h in range(2):
            grad_remote(j, h).wait_send()
            half(j, h).wait_send()
            for k in range(SENDS):
                hop(j, k, h).wait_send()


def on_device(tokens, grads_out, statistics):
    blocks, _, order, piece_width = statistics.shape
    count = lax.axis_size("tok")
    if piece_width != order or count != 2 * LINE or tokens.shape[1] != LINE * order:
        return in_pieces(tokens, grads_out, statistics)
    local, rows, wide, tile = tokens.shape[0], order // 2, order // 2, order // 4
    bf16, f32 = jnp.bfloat16, jnp.float32
    dma = pltpu.SemaphoreType.DMA
    anywhere = pl.BlockSpec(memory_space=pl.ANY)
    square = pltpu.VMEM((order, order), bf16)
    return pl.pallas_call(
        functools.partial(fused_kernel, blocks),
        out_shape=(
            jax.ShapeDtypeStruct((rows, blocks * order), bf16),
            jax.ShapeDtypeStruct(statistics.shape, f32),
        ),
        in_specs=[anywhere] * 3,
        out_specs=(anywhere, anywhere),
        scratch_shapes=[
            pltpu.VMEM((4, 2 * local, rows), bf16),
            pltpu.VMEM((blocks, 2, 2 * local, wide), bf16),
            pltpu.VMEM((blocks, SENDS, 2, rows, wide), bf16),
            pltpu.VMEM((blocks, SLOTS, 2, rows, wide), bf16),
            pltpu.VMEM((2, rows, wide), f32),
            pltpu.VMEM((blocks, order, order), bf16),
            pltpu.VMEM((order, order), f32),
            square,
            square,
            square,
            square,
            pltpu.VMEM((order, order), f32),
            pltpu.VMEM((2, order, order), bf16),
            pltpu.VMEM((rows, order), bf16),
            pltpu.VMEM((rows, order), bf16),
            dma((4,)),
            dma((4,)),
            dma((4,)),
            dma((blocks, 2)),
            dma((blocks, 2)),
            dma((blocks, 2)),
            dma((blocks, SENDS, 2)),
            dma((blocks, SLOTS, 2)),
            dma((blocks, 2)),
            dma((blocks, 2)),
            dma((1,)),
            dma((1,)),
            dma((4,)),
            dma((4,)),
            dma((1,)),
        ],
        compiler_params=pltpu.CompilerParams(
            collective_id=0, has_side_effects=True, vmem_limit_bytes=67043328
        ),
    )(tokens, grads_out, statistics)


def solution(mesh):
    placed = (P("tok", None), P("tok", "col"), P("col", "tok", None, None))
    return jax.shard_map(
        on_device,
        mesh=mesh,
        in_specs=placed,
        out_specs=(P("tok", "col"), P("col", "tok", None, None)),
        check_vma=False,
    )
```

```python
import functools
import math

import jax
import jax.numpy as jnp
from jax import lax
from jax.experimental import pallas as pl
from jax.experimental.pallas import tpu as pltpu
from jax.sharding import PartitionSpec as P

ITERS = 3


def swapped(block, axis, bit):
    count = lax.axis_size(axis)
    route = []
    for low in range(count):
        high = low | 1 << bit
        if high != low and high < count:
            route += [(low, high), (high, low)]
    return lax.ppermute(block, axis, route)


def as_sent(array):
    return jax.tree.map(lambda a: a.astype(jnp.bfloat16) if a.dtype == jnp.float32 else a, array)


def doubling(values, levels, device, axis_dim, partner):
    for level_bit in range(levels):
        partner_part = partner(values, level_bit)
        low_side = device // 2**level_bit % 2 == 0
        values = jnp.where(
            low_side,
            jnp.concatenate([values, partner_part], axis_dim),
            jnp.concatenate([partner_part, values], axis_dim),
        )
    return values


def product(left_side, right_side):
    return jnp.einsum("bij,bjk->bik", left_side, right_side, precision=lax.Precision.HIGHEST)


def in_pieces(tokens, grads_out, statistics):
    device = lax.axis_index("tok")
    blocks = statistics.shape[0]
    order_size = statistics.shape[2]
    piece_width = statistics.shape[3]
    pieces = order_size // piece_width
    levels = pieces.bit_length() - 1
    rows_dev = tokens.shape[1] // lax.axis_size("tok")
    side_bit = device // pieces % 2
    column = device % pieces
    slab_index = device % (2 * pieces)

    def columns_of(values):
        return lax.dynamic_slice_in_dim(values, column * piece_width, piece_width, 2)

    owned = lax.psum_scatter(
        lax.dot_general(
            tokens, grads_out, (((0,), (0,)), ((), ())), preferred_element_type=jnp.float32
        ),
        "tok",
        scatter_dimension=0,
        tiled=True,
    ).astype(jnp.bfloat16)
    gradient = doubling(
        owned, levels + 1, device, 0, lambda portion, level_bit: swapped(portion, "tok", level_bit)
    )
    grad_cube = gradient.reshape(order_size, blocks, order_size)
    forward = jnp.transpose(grad_cube, (1, 0, 2))
    backward = jnp.transpose(grad_cube, (1, 2, 0))
    oriented = jnp.where(side_bit == 0, forward, backward)
    own_rows = lax.dynamic_slice_in_dim(oriented, column * piece_width, piece_width, 1)
    gram_piece = jnp.einsum("brc,bqc->brq", oriented, own_rows, preferred_element_type=jnp.float32)
    fresh_stat = statistics[:, 0] + gram_piece
    identity = jnp.eye(order_size, dtype=jnp.float32)

    def widen(values):
        return doubling(
            values, levels, device, 2, lambda portion, level_bit: swapped(portion, "tok", level_bit)
        )

    assembled = widen(fresh_stat)
    scaling = (2.5 / jnp.sqrt(jnp.sum(assembled * assembled, axis=(1, 2)) + 1e-06))[:, None, None]
    matrix = scaling * assembled
    factor = (5.0 * identity - matrix) * 0.25
    iterate = jnp.sqrt(jnp.sqrt(scaling)) * columns_of(factor)
    for repeat in range(1, ITERS):
        square = widen(product(factor, columns_of(factor)))
        fourth = widen(product(square, columns_of(square)))
        matrix = widen(product(fourth, columns_of(matrix)))
        factor = (5.0 * identity - matrix) * 0.25
        iterate = product(factor, iterate)
    own_root = doubling(
        iterate.astype(jnp.bfloat16),
        levels,
        device,
        2,
        lambda portion, level_bit: jax.tree.map(
            lambda part, own: part.astype(own.dtype),
            swapped(as_sent(portion), "tok", level_bit),
            portion,
        ),
    )
    other_root = swapped(own_root, "tok", levels)
    left_root = jnp.where(side_bit == 0, own_root, other_root)
    right_root = jnp.where(side_bit == 0, other_root, own_root)
    left_rows = lax.dynamic_slice_in_dim(left_root, slab_index * rows_dev, rows_dev, 1)
    mixed_rows = jnp.einsum(
        "bsr,rbc->bsc", left_rows, grad_cube, preferred_element_type=jnp.float32
    ).astype(jnp.bfloat16)
    update = jnp.einsum(
        "bsc,bcd->sbd", mixed_rows, right_root, preferred_element_type=jnp.float32
    ) * math.sqrt(order_size)
    return (update.reshape(rows_dev, blocks * order_size).astype(jnp.bfloat16), fresh_stat[:, None])


LINE = 4
SENDS = 3
SLOTS = 5


def fused_kernel(
    blocks, tokens, grads, old, stats, roots, grad, staged,
    tok2, grad2, sent, got, own32, scaled, one, two, three,
    tok_in, tok_send, tok_recv, grad_in, grad_send, grad_recv, hop_send, hop_recv,
    half_send, half_recv, stat_in, root_send, root_recv,
):
    f32, bf16 = jnp.float32, jnp.bfloat16
    order = grad.shape[1]
    local = tokens.shape[0]
    rows = order // 2
    wide = order // 2
    tile = order // 4
    me = lax.axis_index("tok")
    spot, core = me // 2, lax.rem(me, 2)
    partner = spot * 2 + 1 - core
    outer = jnp.logical_or(spot == 0, spot == LINE - 1)
    inner = jnp.logical_not(outer)
    low = spot < LINE // 2
    near = spot + 1 - 2 * lax.rem(spot, 2)
    across = LINE - 1 - spot
    near_device, across_device = near * 2 + core, across * 2 + core

    def chunk_of(k):
        far = jnp.where(low, LINE - 1 - k, k)
        return jnp.where(k < 2, far, jnp.where(k == 2, near, spot))

    def remote(source, target, send, recv, device):
        return pltpu.make_async_remote_copy(
            src_ref=source, dst_ref=target, send_sem=send, recv_sem=recv,
            device_id={"tok": device}, device_id_type=pl.DeviceIdType.MESH,
        )

    def columns(k, owner):
        return pl.ds(pl.multiple_of((chunk_of(k) * 2 + owner) * rows, rows), rows)

    def tok_local(k):
        return pltpu.make_async_copy(
            tokens.at[:, columns(k, core)], tok2.at[k, pl.ds(0, local), :], tok_in.at[k]
        )

    def tok_remote(k):
        return remote(
            tokens.at[:, columns(k, 1 - core)], tok2.at[k, pl.ds(local, local), :],
            tok_send.at[k], tok_recv.at[k], partner,
        )

    def grad_columns(j, h):
        return pl.ds(pl.multiple_of(j * order + h * wide, wide), wide)

    def grad_local(j, h):
        return pltpu.make_async_copy(
            grads.at[:, grad_columns(j, h)], grad2.at[j, h, pl.ds(0, local), :], grad_in.at[j, h]
        )

    def grad_remote(j, h):
        return remote(
            grads.at[:, grad_columns(j, h)], grad2.at[j, h, pl.ds(local, local), :],
            grad_send.at[j, h], grad_recv.at[j, h], partner,
        )

    def stat_load(j):
        return pltpu.make_async_copy(old.at[j, 0], stats.at[j], stat_in.at[j])

    def hop(j, k, h):
        slot = jnp.where(jnp.logical_or(outer, k == 2), k, SENDS + k)
        device = jnp.where(jnp.logical_or(outer, k == 2), near_device, across_device)
        return remote(
            sent.at[k, h], got.at[j, slot, h], hop_send.at[k, h], hop_recv.at[j, slot, h], device,
        )

    def arrived(j, slot, h):
        remote(
            sent.at[0, h], got.at[j, slot, h], hop_send.at[0, h], hop_recv.at[j, slot, h],
            near_device,
        ).wait_recv()

    def half(j, h):
        part = grad.at[j, pl.ds(pl.multiple_of(core * rows, rows), rows), pl.ds(h * wide, wide)]
        return remote(part, part, half_send.at[j, h], half_recv.at[j, h], partner)

    def half_arrived(j, h):
        part = grad.at[
            j, pl.ds(pl.multiple_of((1 - core) * rows, rows), rows), pl.ds(h * wide, wide)
        ]
        remote(part, part, half_send.at[j, h], half_recv.at[j, h], partner).wait_recv()

    def root_piece(n, side):
        part = roots.at[side, pl.ds(n * tile, tile), :]
        return remote(part, part, root_send.at[n], root_recv.at[n], partner)

    barrier = pltpu.get_barrier_semaphore()
    pl.semaphore_signal(
        barrier, inc=1, device_id={"tok": partner}, device_id_type=pl.DeviceIdType.MESH
    )
    pl.semaphore_signal(
        barrier, inc=1, device_id={"tok": near_device}, device_id_type=pl.DeviceIdType.MESH
    )

    @pl.when(inner)
    def _():
        pl.semaphore_signal(
            barrier, inc=1, device_id={"tok": across_device}, device_id_type=pl.DeviceIdType.MESH
        )

    tok_local(0).start()
    grad_local(0, 0).start()
    pl.semaphore_wait(barrier, jnp.where(inner, 3, 2))
    tok_remote(0).start()
    grad_remote(0, 0).start()
    for h in range(2):
        if h:
            grad_local(0, h).start()
            grad_remote(0, h).start()
    for k in range(1, 4):
        tok_local(k).start()
        tok_remote(k).start()
    for j in range(1, blocks):
        for h in range(2):
            grad_local(j, h).start()
            grad_remote(j, h).start()
    for j in range(blocks):
        stat_load(j).start()

    def wait_tokens(k):
        tok_local(k).wait()
        tok_remote(k).wait_recv()

    def wait_grads(j, h):
        grad_local(j, h).wait()
        grad_remote(j, h).wait_recv()

    def partial(j, k, h):
        return lax.dot_general(
            tok2[k], grad2[j, h], (((0,), (0,)), ((), ())), preferred_element_type=f32
        )

    def step(s, carry):
        j, k = s // SENDS, lax.rem(s, SENDS)

        @pl.when(j == 0)
        def _():
            wait_tokens(k)

        for h in range(2):

            @pl.when(k == 0)
            def _():
                wait_grads(j, h)

            sent_part = partial(j, k, h)

            @pl.when(j > 0)
            def _():
                hop(j - 1, k, h).wait_send()

            @pl.when(outer)
            def _():
                sent[k, h] = sent_part.astype(bf16)

            @pl.when(inner)
            def _():
                slot = jnp.where(k == 2, SENDS, k)
                arrived(j, slot, h)
                sent[k, h] = (sent_part + got[j, slot, h].astype(f32)).astype(bf16)

            hop(j, k, h).start()
        return carry

    def put(ref, n, value):
        value = value.astype(bf16)
        ref[n : n + tile, n:] = value
        if n + tile < order:
            ref[n + tile :, n : n + tile] = value[:, tile:].T

    def product(left, right, finish):
        for n in range(0, order, tile):
            total = jnp.dot(left[n : n + tile, :], right[:, n:], preferred_element_type=f32)
            finish(total, n, (slice(n, n + tile), slice(n, None)))

    def one_block(j, carry):
        stat = stats.at[j]
        split = jnp.where(outer, blocks * SENDS, SENDS)
        lax.fori_loop(
            jnp.where(j == 0, 0, jnp.maximum(split, j * SENDS)),
            jnp.where(j == 0, split, jnp.maximum(split, (j + 1) * SENDS)),
            step,
            0,
        )

        @pl.when(j == 0)
        def _():
            wait_tokens(SENDS)

        for h in range(2):
            own32[h] = partial(j, SENDS, h)
        for h in range(2):
            arrived(j, 2, h)

            @pl.when(outer)
            def _():
                own32[h] = own32[h] + got[j, 2, h].astype(f32)

            @pl.when(inner)
            def _():
                arrived(j, SENDS + 1, h)
                own32[h] = (
                    own32[h] + got[j, 2, h].astype(f32) + got[j, SENDS + 1, h].astype(f32)
                )

            grad[j, pl.ds(pl.multiple_of(core * rows, rows), rows), h * wide : (h + 1) * wide] = (
                own32[h].astype(bf16)
            )
            half(j, h).start()
        stat_load(j).wait()
        for h in range(2):
            half_arrived(j, h)

        def gram(left):
            sums = jnp.zeros((1, order), f32)
            for n in range(0, order, tile):
                if left:
                    total = lax.dot_general(
                        grad[j, n : n + tile, :], grad[j, n:, :], (((1,), (1,)), ((), ())),
                        preferred_element_type=f32,
                    )
                else:
                    total = lax.dot_general(
                        grad[j, :, n : n + tile], grad[j, :, n:], (((0,), (0,)), ((), ())),
                        preferred_element_type=f32,
                    )
                total = total + stat[n : n + tile, n:]
                stat[n : n + tile, n:] = total
                square = jnp.sum(total * total, axis=0, keepdims=True)
                own = jnp.sum(square[:, :tile], axis=1, keepdims=True)
                if n + tile < order:
                    stat[n + tile :, n : n + tile] = total[:, tile:].T
                    own = own + 2.0 * jnp.sum(square[:, tile:], axis=1, keepdims=True)
                sums = sums + own
            own32[0, 0:1, :] = sums[:, :wide]

        pl.when(core == 0)(lambda: gram(True))
        pl.when(core == 1)(lambda: gram(False))
        zeta = 2.5 / jnp.sqrt(own32[0, 0:1, 0:1] + 1e-06)
        gain = jnp.sqrt(jnp.sqrt(zeta))
        scaled[...] = (zeta * stat[...]).astype(bf16)

        def first_square(total, n, at):
            put(one, n, (total - 10.0 * scaled[at].astype(f32)) * 0.0625)

        product(scaled, scaled, first_square)

        def first_fourth(total, n, at):
            put(two, n, 3.125 * one[at].astype(f32) + total)

        product(one, one, first_fourth)

        def second(total, n, at):
            put(three, n, (2.44140625 * zeta) * stat[at] + total)

        product(two, scaled, second)

        def second_square(total, n, at):
            base = three[at].astype(f32)
            put(one, n, (total - 10.0 * base) * 0.0625)
            put(two, n, (5.0 * base - total) * 0.25)

        product(three, three, second_square)
        mine = roots.at[core]

        def second_fourth(total, n, at):
            put(mine, n, 3.125 * one[at].astype(f32) + total)

        product(one, one, second_fourth)

        def factors(total, n, at):
            value = -0.25 * (
                1.25 * three[at].astype(f32) + 2.44140625 * two[at].astype(f32) + total
            )
            put(one, n, value)
            three[at] = (value - value.astype(bf16).astype(f32)).astype(bf16)

        product(mine, two, factors)

        def final(total, n, at):
            shape = total.shape
            unit = (
                lax.broadcasted_iota(jnp.int32, shape, 0)
                == lax.broadcasted_iota(jnp.int32, shape, 1)
            ).astype(f32)
            rest = one[at].astype(f32) + three[at].astype(f32)
            value = 1.953125 * unit + 1.25 * rest - (0.390625 * zeta) * stat[at] - 0.25 * total
            put(mine, n, gain * value)
            root_piece(n // tile, core).start()

        product(one, scaled, final)

        def roots_arrived():
            for n in range(4):
                root_piece(n, 1 - core).wait_recv()

        last = j == blocks - 1
        pl.when(jnp.logical_or(core == 1, last))(roots_arrived)

        @pl.when(jnp.logical_not(last))
        def _():
            left = roots[0, pl.ds(pl.multiple_of(core * rows, rows), rows), :]
            three[:rows] = jnp.dot(left, grad[j], preferred_element_type=f32).astype(bf16)
            pl.when(core == 0)(roots_arrived)
            staged[j] = (
                jnp.dot(three[:rows], roots[1], preferred_element_type=f32) * math.sqrt(order)
            ).astype(bf16)

        for n in range(4):
            root_piece(n, core).wait_send()
        return carry

    lax.fori_loop(0, blocks, one_block, 0)
    for k in range(4):
        tok_remote(k).wait_send()
    for j in range(blocks):
        for h in range(2):
            grad_remote(j, h).wait_send()
            half(j, h).wait_send()
    for h in range(2):
        for k in range(SENDS):
            hop(blocks - 1, k, h).wait_send()


def last_kernel(blocks, stats, roots, grad, staged, update, fresh, mixed, final, sems):
    f32, bf16 = jnp.float32, jnp.bfloat16
    order = grad.shape[1]
    rows = order // 2
    core = lax.rem(lax.axis_index("tok"), 2)
    copies = [
        pltpu.make_async_copy(stats.at[j], fresh.at[j, 0], sems.at[j]) for j in range(blocks)
    ]
    copies += [
        pltpu.make_async_copy(
            staged.at[j], update.at[:, j * order : (j + 1) * order], sems.at[blocks + j]
        )
        for j in range(blocks - 1)
    ]
    for copy in copies:
        copy.start()
    left = roots[0, pl.ds(pl.multiple_of(core * rows, rows), rows), :]
    mixed[...] = jnp.dot(left, grad[blocks - 1], preferred_element_type=f32).astype(bf16)
    for h in range(2):
        half = slice(h * (rows // 2), (h + 1) * (rows // 2))
        final[half] = (
            jnp.dot(mixed[half], roots[1], preferred_element_type=f32) * math.sqrt(order)
        ).astype(bf16)
        copy = pltpu.make_async_copy(
            final.at[half], update.at[half, (blocks - 1) * order :], sems.at[2 * blocks - 1 + h]
        )
        copy.start()
        copies.append(copy)
    for copy in copies:
        copy.wait()


def on_device(tokens, grads_out, statistics):
    blocks, _, order, piece_width = statistics.shape
    count = lax.axis_size("tok")
    if piece_width != order or count != 2 * LINE or tokens.shape[1] != LINE * order:
        return in_pieces(tokens, grads_out, statistics)
    local, rows, wide, tile = tokens.shape[0], order // 2, order // 2, order // 4
    bf16, f32 = jnp.bfloat16, jnp.float32
    dma = pltpu.SemaphoreType.DMA
    anywhere = pl.BlockSpec(memory_space=pl.ANY)
    near = pl.BlockSpec(memory_space=pltpu.VMEM)
    square = pltpu.VMEM((order, order), bf16)
    held = pl.pallas_call(
        functools.partial(fused_kernel, blocks),
        out_shape=(
            pltpu.VMEM((blocks, order, order), f32),
            pltpu.VMEM((2, order, order), bf16),
            pltpu.VMEM((blocks, order, order), bf16),
            pltpu.VMEM((max(blocks - 1, 1), rows, order), bf16),
        ),
        in_specs=[anywhere] * 3,
        out_specs=(near,) * 4,
        scratch_shapes=[
            pltpu.VMEM((4, 2 * local, rows), bf16),
            pltpu.VMEM((blocks, 2, 2 * local, wide), bf16),
            pltpu.VMEM((SENDS, 2, rows, wide), bf16),
            pltpu.VMEM((blocks, SLOTS, 2, rows, wide), bf16),
            pltpu.VMEM((2, rows, wide), f32),
            square,
            square,
            square,
            square,
            dma((4,)),
            dma((4,)),
            dma((4,)),
            dma((blocks, 2)),
            dma((blocks, 2)),
            dma((blocks, 2)),
            dma((SENDS, 2)),
            dma((blocks, SLOTS, 2)),
            dma((blocks, 2)),
            dma((blocks, 2)),
            dma((blocks,)),
            dma((4,)),
            dma((4,)),
        ],
        compiler_params=pltpu.CompilerParams(
            collective_id=0, has_side_effects=True, vmem_limit_bytes=46 << 20
        ),
    )(tokens, grads_out, statistics)
    return pl.pallas_call(
        functools.partial(last_kernel, blocks),
        out_shape=(
            jax.ShapeDtypeStruct((rows, blocks * order), bf16),
            jax.ShapeDtypeStruct(statistics.shape, f32),
        ),
        in_specs=[near] * 4,
        out_specs=(anywhere, anywhere),
        scratch_shapes=[
            pltpu.VMEM((rows, order), bf16),
            pltpu.VMEM((rows, order), bf16),
            dma((2 * blocks + 1,)),
        ],
        compiler_params=pltpu.CompilerParams(vmem_limit_bytes=24 << 20),
    )(*held)


def solution(mesh):
    placed = (P("tok", None), P("tok", "col"), P("col", "tok", None, None))
    return jax.shard_map(
        on_device,
        mesh=mesh,
        in_specs=placed,
        out_specs=(P("tok", "col"), P("col", "tok", None, None)),
        check_vma=False,
    )
```

```python
import functools
import math

import jax
import jax.numpy as jnp
from jax import lax
from jax.experimental import pallas as pl
from jax.experimental.pallas import tpu as pltpu
from jax.sharding import PartitionSpec as P

ITERS = 3


def swapped(block, axis, bit):
    count = lax.axis_size(axis)
    route = []
    for low in range(count):
        high = low | 1 << bit
        if high != low and high < count:
            route += [(low, high), (high, low)]
    return lax.ppermute(block, axis, route)


def as_sent(array):
    return jax.tree.map(lambda a: a.astype(jnp.bfloat16) if a.dtype == jnp.float32 else a, array)


def doubling(values, levels, device, axis_dim, partner):
    for level_bit in range(levels):
        partner_part = partner(values, level_bit)
        low_side = device // 2**level_bit % 2 == 0
        values = jnp.where(
            low_side,
            jnp.concatenate([values, partner_part], axis_dim),
            jnp.concatenate([partner_part, values], axis_dim),
        )
    return values


def product(left_side, right_side):
    return jnp.einsum("bij,bjk->bik", left_side, right_side, precision=lax.Precision.HIGHEST)


def in_pieces(tokens, grads_out, statistics):
    device = lax.axis_index("tok")
    blocks = statistics.shape[0]
    order_size = statistics.shape[2]
    piece_width = statistics.shape[3]
    pieces = order_size // piece_width
    levels = pieces.bit_length() - 1
    rows_dev = tokens.shape[1] // lax.axis_size("tok")
    side_bit = device // pieces % 2
    column = device % pieces
    slab_index = device % (2 * pieces)

    def columns_of(values):
        return lax.dynamic_slice_in_dim(values, column * piece_width, piece_width, 2)

    owned = lax.psum_scatter(
        lax.dot_general(
            tokens, grads_out, (((0,), (0,)), ((), ())), preferred_element_type=jnp.float32
        ),
        "tok",
        scatter_dimension=0,
        tiled=True,
    ).astype(jnp.bfloat16)
    gradient = doubling(
        owned, levels + 1, device, 0, lambda portion, level_bit: swapped(portion, "tok", level_bit)
    )
    grad_cube = gradient.reshape(order_size, blocks, order_size)
    forward = jnp.transpose(grad_cube, (1, 0, 2))
    backward = jnp.transpose(grad_cube, (1, 2, 0))
    oriented = jnp.where(side_bit == 0, forward, backward)
    own_rows = lax.dynamic_slice_in_dim(oriented, column * piece_width, piece_width, 1)
    gram_piece = jnp.einsum("brc,bqc->brq", oriented, own_rows, preferred_element_type=jnp.float32)
    fresh_stat = statistics[:, 0] + gram_piece
    identity = jnp.eye(order_size, dtype=jnp.float32)

    def widen(values):
        return doubling(
            values, levels, device, 2, lambda portion, level_bit: swapped(portion, "tok", level_bit)
        )

    assembled = widen(fresh_stat)
    scaling = (2.5 / jnp.sqrt(jnp.sum(assembled * assembled, axis=(1, 2)) + 1e-06))[:, None, None]
    matrix = scaling * assembled
    factor = (5.0 * identity - matrix) * 0.25
    iterate = jnp.sqrt(jnp.sqrt(scaling)) * columns_of(factor)
    for repeat in range(1, ITERS):
        square = widen(product(factor, columns_of(factor)))
        fourth = widen(product(square, columns_of(square)))
        matrix = widen(product(fourth, columns_of(matrix)))
        factor = (5.0 * identity - matrix) * 0.25
        iterate = product(factor, iterate)
    own_root = doubling(
        iterate.astype(jnp.bfloat16),
        levels,
        device,
        2,
        lambda portion, level_bit: jax.tree.map(
            lambda part, own: part.astype(own.dtype),
            swapped(as_sent(portion), "tok", level_bit),
            portion,
        ),
    )
    other_root = swapped(own_root, "tok", levels)
    left_root = jnp.where(side_bit == 0, own_root, other_root)
    right_root = jnp.where(side_bit == 0, other_root, own_root)
    left_rows = lax.dynamic_slice_in_dim(left_root, slab_index * rows_dev, rows_dev, 1)
    mixed_rows = jnp.einsum(
        "bsr,rbc->bsc", left_rows, grad_cube, preferred_element_type=jnp.float32
    ).astype(jnp.bfloat16)
    update = jnp.einsum(
        "bsc,bcd->sbd", mixed_rows, right_root, preferred_element_type=jnp.float32
    ) * math.sqrt(order_size)
    return (update.reshape(rows_dev, blocks * order_size).astype(jnp.bfloat16), fresh_stat[:, None])


LINE = 4
SENDS = 3
SLOTS = 5
PIECES = 4


def fused_kernel(
    blocks, tokens, grads, old, stats, roots, grad, staged,
    tok2, grad2, sent, got, own32, scaled, one, two, three,
    tok_in, tok_send, tok_recv, grad_in, grad_send, grad_recv, hop_send, hop_recv,
    half_send, half_recv, stat_in, root_send, root_recv,
):
    f32, bf16 = jnp.float32, jnp.bfloat16
    order = grad.shape[1]
    local = tokens.shape[0]
    rows = order // 2
    wide = tile = order // PIECES
    me = lax.axis_index("tok")
    spot, core = me // 2, lax.rem(me, 2)
    partner = spot * 2 + 1 - core
    outer = jnp.logical_or(spot == 0, spot == LINE - 1)
    inner = jnp.logical_not(outer)
    low = spot < LINE // 2
    near = spot + 1 - 2 * lax.rem(spot, 2)
    across = LINE - 1 - spot
    near_device, across_device = near * 2 + core, across * 2 + core

    def chunk_of(k):
        far = jnp.where(low, LINE - 1 - k, k)
        return jnp.where(k < 2, far, jnp.where(k == 2, near, spot))

    def remote(source, target, send, recv, device):
        return pltpu.make_async_remote_copy(
            src_ref=source, dst_ref=target, send_sem=send, recv_sem=recv,
            device_id={"tok": device}, device_id_type=pl.DeviceIdType.MESH,
        )

    def columns(k, owner):
        return pl.ds(pl.multiple_of((chunk_of(k) * 2 + owner) * rows, rows), rows)

    def tok_local(k):
        return pltpu.make_async_copy(
            tokens.at[:, columns(k, core)], tok2.at[k, pl.ds(0, local), :], tok_in.at[k]
        )

    def tok_remote(k):
        return remote(
            tokens.at[:, columns(k, 1 - core)], tok2.at[k, pl.ds(local, local), :],
            tok_send.at[k], tok_recv.at[k], partner,
        )

    def grad_columns(j, h):
        return pl.ds(pl.multiple_of(j * order + h * wide, wide), wide)

    def grad_local(j, h):
        return pltpu.make_async_copy(
            grads.at[:, grad_columns(j, h)], grad2.at[j, h, pl.ds(0, local), :], grad_in.at[j, h]
        )

    def grad_remote(j, h):
        return remote(
            grads.at[:, grad_columns(j, h)], grad2.at[j, h, pl.ds(local, local), :],
            grad_send.at[j, h], grad_recv.at[j, h], partner,
        )

    def stat_load(j):
        return pltpu.make_async_copy(old.at[j, 0], stats.at[j], stat_in.at[j])

    def hop(j, k, h):
        slot = jnp.where(jnp.logical_or(outer, k == 2), k, SENDS + k)
        device = jnp.where(jnp.logical_or(outer, k == 2), near_device, across_device)
        return remote(
            sent.at[k, h], got.at[j, slot, h], hop_send.at[k, h], hop_recv.at[j, slot, h], device,
        )

    def arrived(j, slot, h):
        remote(
            sent.at[0, h], got.at[j, slot, h], hop_send.at[0, h], hop_recv.at[j, slot, h],
            near_device,
        ).wait_recv()

    def half(j, h):
        part = grad.at[j, pl.ds(pl.multiple_of(core * rows, rows), rows), pl.ds(h * wide, wide)]
        return remote(part, part, half_send.at[j, h], half_recv.at[j, h], partner)

    def half_arrived(j, h):
        part = grad.at[
            j, pl.ds(pl.multiple_of((1 - core) * rows, rows), rows), pl.ds(h * wide, wide)
        ]
        remote(part, part, half_send.at[j, h], half_recv.at[j, h], partner).wait_recv()

    def root_parts(n, side):
        first, past = n * tile, (n + 1) * tile
        parts = [roots.at[side, first:past, first:]]
        if past < order:
            parts.append(roots.at[side, past:, first:past])
        return [
            remote(part, part, root_send.at[n, i], root_recv.at[n, i], partner)
            for i, part in enumerate(parts)
        ]

    barrier = pltpu.get_barrier_semaphore()
    pl.semaphore_signal(
        barrier, inc=1, device_id={"tok": partner}, device_id_type=pl.DeviceIdType.MESH
    )
    pl.semaphore_signal(
        barrier, inc=1, device_id={"tok": near_device}, device_id_type=pl.DeviceIdType.MESH
    )

    @pl.when(inner)
    def _():
        pl.semaphore_signal(
            barrier, inc=1, device_id={"tok": across_device}, device_id_type=pl.DeviceIdType.MESH
        )

    tok_local(0).start()
    for h in range(PIECES):
        grad_local(0, h).start()
    pl.semaphore_wait(barrier, jnp.where(inner, 3, 2))
    tok_remote(0).start()
    for h in range(PIECES):
        grad_remote(0, h).start()

    def wait_tokens(k):
        tok_local(k).wait()
        tok_remote(k).wait_recv()

    def wait_grads(j, h):
        grad_local(j, h).wait()
        grad_remote(j, h).wait_recv()

    def partial(j, k, h):
        return lax.dot_general(
            tok2[k], grad2[j, h], (((0,), (0,)), ((), ())), preferred_element_type=f32
        )

    def piece(j, k, h):
        @pl.when(k == 0)
        def _():
            wait_grads(j, h)

        sent_part = partial(j, k, h)

        @pl.when(j > 0)
        def _():
            hop(j - 1, k, h).wait_send()

        @pl.when(outer)
        def _():
            sent[k, h] = sent_part.astype(bf16)

        @pl.when(inner)
        def _():
            slot = jnp.where(k == 2, SENDS, k)
            arrived(j, slot, h)
            sent[k, h] = (sent_part + got[j, slot, h].astype(f32)).astype(bf16)

        hop(j, k, h).start()

    def step(s, carry):
        j, r = s // SENDS, lax.rem(s, SENDS)
        k = jnp.where(outer, r, lax.rem(SENDS - r, SENDS))

        @pl.when(j == 0)
        def _():
            wait_tokens(k)

        for h in range(PIECES):
            piece(j, k, h)

        @pl.when(s == 0)
        def _():
            for later in range(1, 4):
                tok_local(later).start()
                tok_remote(later).start()

        @pl.when(s == 1)
        def _():
            for later in range(1, blocks):
                for h in range(PIECES):
                    grad_local(later, h).start()
                    grad_remote(later, h).start()
            for later in range(blocks):
                stat_load(later).start()

        return carry

    def put(ref, n, value):
        value = value.astype(bf16)
        ref[n : n + tile, n:] = value
        if n + tile < order:
            ref[n + tile :, n : n + tile] = value[:, tile:].T

    def product(left, right, finish):
        for n in range(0, order, tile):
            total = jnp.dot(left[n : n + tile, :], right[:, n:], preferred_element_type=f32)
            finish(total, n, (slice(n, n + tile), slice(n, None)))

    def one_block(j, carry):
        stat = stats.at[j]
        last = j == blocks - 1
        split = blocks * SENDS
        first = jnp.where(outer, jnp.where(j == 0, 0, split), j * SENDS + jnp.minimum(j, 1))
        end = jnp.where(outer, split, (j + 1) * SENDS)
        lax.fori_loop(first, end, step, 0)

        @pl.when(j == 0)
        def _():
            wait_tokens(SENDS)

        def ahead(h):
            @pl.when(jnp.logical_and(inner, jnp.logical_not(last)))
            def _():
                piece(j + 1, 0, h)

        for h in range(PIECES):
            own32[h] = partial(j, SENDS, h)
        stat_load(j).wait()

        def norm(total, own, other):
            square = jnp.sum(total * total, axis=0, keepdims=True)
            value = jnp.sum(square[:, own], axis=1, keepdims=True)
            if other is not None:
                value = value + 2.0 * jnp.sum(square[:, other], axis=1, keepdims=True)
            return value

        def gram_left(h):
            columns = slice(h * wide, (h + 1) * wide)
            sums = jnp.zeros((1, 1), f32)
            for n in range(0, order, tile):
                at = (slice(n, n + tile), slice(n, None))
                total = stat[at] + lax.dot_general(
                    grad[j, n : n + tile, columns], grad[j, n:, columns],
                    (((1,), (1,)), ((), ())), preferred_element_type=f32,
                )
                stat[at] = total
                if h == PIECES - 1:
                    put(scaled, n, total)
                    rest = slice(tile, None) if n + tile < order else None
                    sums = sums + norm(total, slice(0, tile), rest)
            if h == PIECES - 1:
                own32[0, 0:1, 0:wide] = jnp.broadcast_to(sums, (1, wide))

        def gram_right(h):
            n, reach = h * tile, (h + 1) * tile
            total = stat[:reach, n:reach] + lax.dot_general(
                grad[j, :, :reach], grad[j, :, n:reach], (((0,), (0,)), ((), ())),
                preferred_element_type=f32,
            )
            stat[:reach, n:reach] = total
            scaled[:reach, n:reach] = total.astype(bf16)
            diagonal = total[n:]
            sums = jnp.sum(jnp.sum(diagonal * diagonal, axis=0, keepdims=True), axis=1, keepdims=True)
            if h:
                above = total[:n]
                scaled[n:reach, :n] = above.astype(bf16).T
                sums = sums + 2.0 * jnp.sum(
                    jnp.sum(above * above, axis=0, keepdims=True), axis=1, keepdims=True
                )
                sums = sums + own32[0, 0:1, 0:1]
            own32[0, 0:1, 0:wide] = jnp.broadcast_to(sums, (1, wide))

        for h in range(PIECES):
            arrived(j, 2, h)

            @pl.when(outer)
            def _():
                own32[h] = own32[h] + got[j, 2, h].astype(f32)

            @pl.when(inner)
            def _():
                arrived(j, SENDS + 1, h)
                own32[h] = (
                    own32[h] + got[j, 2, h].astype(f32) + got[j, SENDS + 1, h].astype(f32)
                )

            grad[j, pl.ds(pl.multiple_of(core * rows, rows), rows), h * wide : (h + 1) * wide] = (
                own32[h].astype(bf16)
            )
            half(j, h).start()
            half_arrived(j, h)
            pl.when(core == 0)(functools.partial(gram_left, h))
            pl.when(core == 1)(functools.partial(gram_right, h))

        zeta = 2.5 / jnp.sqrt(own32[0, 0:1, 0:1] + 1e-06)
        gain = jnp.sqrt(jnp.sqrt(zeta))

        def first_square(total, n, at):
            put(one, n, (zeta * zeta * 0.0625) * total - (0.625 * zeta) * stat[at])
            if n + tile < order:
                stat[n + tile :, n : n + tile] = stat[n : n + tile, n + tile :].T

        product(scaled, scaled, first_square)
        ahead(0)

        def first_fourth(total, n, at):
            put(two, n, 3.125 * one[at].astype(f32) + total)

        product(one, one, first_fourth)

        def second(total, n, at):
            put(three, n, zeta * (2.44140625 * stat[at] + total))

        product(two, scaled, second)
        ahead(1)

        def second_square(total, n, at):
            base = three[at].astype(f32)
            put(one, n, (total - 10.0 * base) * 0.0625)
            put(two, n, (5.0 * base - total) * 0.25)

        product(three, three, second_square)
        mine = roots.at[core]

        def second_fourth(total, n, at):
            put(mine, n, 3.125 * one[at].astype(f32) + total)

        product(one, one, second_fourth)
        ahead(2)

        def factors(total, n, at):
            value = -0.25 * (
                1.25 * three[at].astype(f32) + 2.44140625 * two[at].astype(f32) + total
            )
            put(one, n, value)
            three[at] = (value - value.astype(bf16).astype(f32)).astype(bf16)

        product(mine, two, factors)

        def final(total, n, at):
            shape = total.shape
            unit = (
                lax.broadcasted_iota(jnp.int32, shape, 0)
                == lax.broadcasted_iota(jnp.int32, shape, 1)
            ).astype(f32)
            rest = one[at].astype(f32) + three[at].astype(f32)
            value = 1.953125 * unit + 1.25 * rest - zeta * (0.390625 * stat[at] + 0.25 * total)
            put(mine, n, gain * value)
            for part in root_parts(n // tile, core):
                part.start()

        product(one, scaled, final)
        ahead(3)

        def roots_arrived():
            for n in range(PIECES):
                for part in root_parts(n, 1 - core):
                    part.wait_recv()

        pl.when(jnp.logical_or(core == 1, last))(roots_arrived)

        @pl.when(jnp.logical_not(last))
        def _():
            left = roots[0, pl.ds(pl.multiple_of(core * rows, rows), rows), :]
            three[:rows] = jnp.dot(left, grad[j], preferred_element_type=f32).astype(bf16)
            pl.when(core == 0)(roots_arrived)
            staged[j] = (
                jnp.dot(three[:rows], roots[1], preferred_element_type=f32) * math.sqrt(order)
            ).astype(bf16)

        for n in range(PIECES):
            for part in root_parts(n, core):
                part.wait_send()
        return carry

    lax.fori_loop(0, blocks, one_block, 0)
    for k in range(4):
        tok_remote(k).wait_send()
    for h in range(PIECES):
        for j in range(blocks):
            grad_remote(j, h).wait_send()
            half(j, h).wait_send()
        for k in range(SENDS):
            hop(blocks - 1, k, h).wait_send()


def last_kernel(blocks, stats, roots, grad, staged, update, fresh, mixed, final, sems):
    f32, bf16 = jnp.float32, jnp.bfloat16
    order = grad.shape[1]
    rows = order // 2
    core = lax.rem(lax.axis_index("tok"), 2)
    copies = [
        pltpu.make_async_copy(stats.at[j], fresh.at[j, 0], sems.at[j]) for j in range(blocks)
    ]
    copies += [
        pltpu.make_async_copy(
            staged.at[j], update.at[:, j * order : (j + 1) * order], sems.at[blocks + j]
        )
        for j in range(blocks - 1)
    ]
    for copy in copies:
        copy.start()
    left = roots[0, pl.ds(pl.multiple_of(core * rows, rows), rows), :]
    mixed[...] = jnp.dot(left, grad[blocks - 1], preferred_element_type=f32).astype(bf16)
    for h in range(2):
        half = slice(h * (rows // 2), (h + 1) * (rows // 2))
        final[half] = (
            jnp.dot(mixed[half], roots[1], preferred_element_type=f32) * math.sqrt(order)
        ).astype(bf16)
        copy = pltpu.make_async_copy(
            final.at[half], update.at[half, (blocks - 1) * order :], sems.at[2 * blocks - 1 + h]
        )
        copy.start()
        copies.append(copy)
    for copy in copies:
        copy.wait()


def on_device(tokens, grads_out, statistics):
    blocks, _, order, piece_width = statistics.shape
    count = lax.axis_size("tok")
    if piece_width != order or count != 2 * LINE or tokens.shape[1] != LINE * order:
        return in_pieces(tokens, grads_out, statistics)
    local, rows, wide = tokens.shape[0], order // 2, order // PIECES
    bf16, f32 = jnp.bfloat16, jnp.float32
    dma = pltpu.SemaphoreType.DMA
    anywhere = pl.BlockSpec(memory_space=pl.ANY)
    near = pl.BlockSpec(memory_space=pltpu.VMEM)
    square = pltpu.VMEM((order, order), bf16)
    held = pl.pallas_call(
        functools.partial(fused_kernel, blocks),
        out_shape=(
            pltpu.VMEM((blocks, order, order), f32),
            pltpu.VMEM((2, order, order), bf16),
            pltpu.VMEM((blocks, order, order), bf16),
            pltpu.VMEM((max(blocks - 1, 1), rows, order), bf16),
        ),
        in_specs=[anywhere] * 3,
        out_specs=(near,) * 4,
        scratch_shapes=[
            pltpu.VMEM((4, 2 * local, rows), bf16),
            pltpu.VMEM((blocks, PIECES, 2 * local, wide), bf16),
            pltpu.VMEM((SENDS, PIECES, rows, wide), bf16),
            pltpu.VMEM((blocks, SLOTS, PIECES, rows, wide), bf16),
            pltpu.VMEM((PIECES, rows, wide), f32),
            square,
            square,
            square,
            square,
            dma((4,)),
            dma((4,)),
            dma((4,)),
            dma((blocks, PIECES)),
            dma((blocks, PIECES)),
            dma((blocks, PIECES)),
            dma((SENDS, PIECES)),
            dma((blocks, SLOTS, PIECES)),
            dma((blocks, PIECES)),
            dma((blocks, PIECES)),
            dma((blocks,)),
            dma((PIECES, 2)),
            dma((PIECES, 2)),
        ],
        compiler_params=pltpu.CompilerParams(
            collective_id=0, has_side_effects=True, vmem_limit_bytes=46 << 20
        ),
    )(tokens, grads_out, statistics)
    return pl.pallas_call(
        functools.partial(last_kernel, blocks),
        out_shape=(
            jax.ShapeDtypeStruct((rows, blocks * order), bf16),
            jax.ShapeDtypeStruct(statistics.shape, f32),
        ),
        in_specs=[near] * 4,
        out_specs=(anywhere, anywhere),
        scratch_shapes=[
            pltpu.VMEM((rows, order), bf16),
            pltpu.VMEM((rows, order), bf16),
            dma((2 * blocks + 1,)),
        ],
        compiler_params=pltpu.CompilerParams(vmem_limit_bytes=24 << 20),
    )(*held)


def solution(mesh):
    placed = (P("tok", None), P("tok", "col"), P("col", "tok", None, None))
    return jax.shard_map(
        on_device,
        mesh=mesh,
        in_specs=placed,
        out_specs=(P("tok", "col"), P("col", "tok", None, None)),
        check_vma=False,
    )
```

```python
import functools
import math

import jax
import jax.numpy as jnp
from jax import lax
from jax.experimental import pallas as pl
from jax.experimental.pallas import tpu as pltpu
from jax.sharding import PartitionSpec as P

ITERS = 3


def swapped(block, axis, bit):
    count = lax.axis_size(axis)
    route = []
    for low in range(count):
        high = low | 1 << bit
        if high != low and high < count:
            route += [(low, high), (high, low)]
    return lax.ppermute(block, axis, route)


def as_sent(array):
    return jax.tree.map(lambda a: a.astype(jnp.bfloat16) if a.dtype == jnp.float32 else a, array)


def doubling(values, levels, device, axis_dim, partner):
    for level_bit in range(levels):
        partner_part = partner(values, level_bit)
        low_side = device // 2**level_bit % 2 == 0
        values = jnp.where(
            low_side,
            jnp.concatenate([values, partner_part], axis_dim),
            jnp.concatenate([partner_part, values], axis_dim),
        )
    return values


def product(left_side, right_side):
    return jnp.einsum("bij,bjk->bik", left_side, right_side, precision=lax.Precision.HIGHEST)


def in_pieces(tokens, grads_out, statistics):
    device = lax.axis_index("tok")
    blocks = statistics.shape[0]
    order_size = statistics.shape[2]
    piece_width = statistics.shape[3]
    pieces = order_size // piece_width
    levels = pieces.bit_length() - 1
    rows_dev = tokens.shape[1] // lax.axis_size("tok")
    side_bit = device // pieces % 2
    column = device % pieces
    slab_index = device % (2 * pieces)

    def columns_of(values):
        return lax.dynamic_slice_in_dim(values, column * piece_width, piece_width, 2)

    owned = lax.psum_scatter(
        lax.dot_general(
            tokens, grads_out, (((0,), (0,)), ((), ())), preferred_element_type=jnp.float32
        ),
        "tok",
        scatter_dimension=0,
        tiled=True,
    ).astype(jnp.bfloat16)
    gradient = doubling(
        owned, levels + 1, device, 0, lambda portion, level_bit: swapped(portion, "tok", level_bit)
    )
    grad_cube = gradient.reshape(order_size, blocks, order_size)
    forward = jnp.transpose(grad_cube, (1, 0, 2))
    backward = jnp.transpose(grad_cube, (1, 2, 0))
    oriented = jnp.where(side_bit == 0, forward, backward)
    own_rows = lax.dynamic_slice_in_dim(oriented, column * piece_width, piece_width, 1)
    gram_piece = jnp.einsum("brc,bqc->brq", oriented, own_rows, preferred_element_type=jnp.float32)
    fresh_stat = statistics[:, 0] + gram_piece
    identity = jnp.eye(order_size, dtype=jnp.float32)

    def widen(values):
        return doubling(
            values, levels, device, 2, lambda portion, level_bit: swapped(portion, "tok", level_bit)
        )

    assembled = widen(fresh_stat)
    scaling = (2.5 / jnp.sqrt(jnp.sum(assembled * assembled, axis=(1, 2)) + 1e-06))[:, None, None]
    matrix = scaling * assembled
    factor = (5.0 * identity - matrix) * 0.25
    iterate = jnp.sqrt(jnp.sqrt(scaling)) * columns_of(factor)
    for repeat in range(1, ITERS):
        square = widen(product(factor, columns_of(factor)))
        fourth = widen(product(square, columns_of(square)))
        matrix = widen(product(fourth, columns_of(matrix)))
        factor = (5.0 * identity - matrix) * 0.25
        iterate = product(factor, iterate)
    own_root = doubling(
        iterate.astype(jnp.bfloat16),
        levels,
        device,
        2,
        lambda portion, level_bit: jax.tree.map(
            lambda part, own: part.astype(own.dtype),
            swapped(as_sent(portion), "tok", level_bit),
            portion,
        ),
    )
    other_root = swapped(own_root, "tok", levels)
    left_root = jnp.where(side_bit == 0, own_root, other_root)
    right_root = jnp.where(side_bit == 0, other_root, own_root)
    left_rows = lax.dynamic_slice_in_dim(left_root, slab_index * rows_dev, rows_dev, 1)
    mixed_rows = jnp.einsum(
        "bsr,rbc->bsc", left_rows, grad_cube, preferred_element_type=jnp.float32
    ).astype(jnp.bfloat16)
    update = jnp.einsum(
        "bsc,bcd->sbd", mixed_rows, right_root, preferred_element_type=jnp.float32
    ) * math.sqrt(order_size)
    return (update.reshape(rows_dev, blocks * order_size).astype(jnp.bfloat16), fresh_stat[:, None])


LINE = 4
SENDS = 3
SLOTS = 5
PIECES = 4
HALVES = 2


def fused_kernel(
    blocks, tokens, grads, old, stats, roots, grad, staged,
    tok2, grad2, sent, got, own32, scaled, one, two, three,
    tok_in, tok_send, tok_recv, grad_in, grad_send, grad_recv, hop_send, hop_recv,
    half_send, half_recv, stat_in, root_send, root_recv,
):
    f32, bf16 = jnp.float32, jnp.bfloat16
    order = grad.shape[1]
    local = tokens.shape[0]
    rows = order // 2
    part_rows = rows // HALVES
    wide = tile = order // PIECES
    me = lax.axis_index("tok")
    spot, core = me // 2, lax.rem(me, 2)
    partner = spot * 2 + 1 - core
    outer = jnp.logical_or(spot == 0, spot == LINE - 1)
    inner = jnp.logical_not(outer)
    low = spot < LINE // 2
    near = spot + 1 - 2 * lax.rem(spot, 2)
    across = LINE - 1 - spot
    near_device, across_device = near * 2 + core, across * 2 + core

    def chunk_of(k):
        far = jnp.where(low, LINE - 1 - k, k)
        return jnp.where(k < 2, far, jnp.where(k == 2, near, spot))

    def remote(source, target, send, recv, device):
        return pltpu.make_async_remote_copy(
            src_ref=source, dst_ref=target, send_sem=send, recv_sem=recv,
            device_id={"tok": device}, device_id_type=pl.DeviceIdType.MESH,
        )

    def columns(k, r, owner):
        start = (chunk_of(k) * 2 + owner) * rows + r * part_rows
        return pl.ds(pl.multiple_of(start, part_rows), part_rows)

    def tok_local(k, r):
        return pltpu.make_async_copy(
            tokens.at[:, columns(k, r, core)], tok2.at[k, r, pl.ds(0, local), :], tok_in.at[k, r]
        )

    def tok_remote(k, r):
        return remote(
            tokens.at[:, columns(k, r, 1 - core)], tok2.at[k, r, pl.ds(local, local), :],
            tok_send.at[k, r], tok_recv.at[k, r], partner,
        )

    def grad_columns(j, h):
        return pl.ds(pl.multiple_of(j * order + h * wide, wide), wide)

    def grad_local(j, h):
        return pltpu.make_async_copy(
            grads.at[:, grad_columns(j, h)], grad2.at[j, h, pl.ds(0, local), :], grad_in.at[j, h]
        )

    def grad_remote(j, h):
        return remote(
            grads.at[:, grad_columns(j, h)], grad2.at[j, h, pl.ds(local, local), :],
            grad_send.at[j, h], grad_recv.at[j, h], partner,
        )

    def stat_load(j):
        return pltpu.make_async_copy(old.at[j, 0], stats.at[j], stat_in.at[j])

    def hop(j, k, h, r):
        slot = jnp.where(jnp.logical_or(outer, k == 2), k, SENDS + k)
        device = jnp.where(jnp.logical_or(outer, k == 2), near_device, across_device)
        return remote(
            sent.at[k, h, r], got.at[j, slot, h, r], hop_send.at[k, h, r],
            hop_recv.at[j, slot, h, r], device,
        )

    def arrived(j, slot, h, r):
        remote(
            sent.at[0, h, r], got.at[j, slot, h, r], hop_send.at[0, h, r],
            hop_recv.at[j, slot, h, r], near_device,
        ).wait_recv()

    def rows_of(owner, r):
        start = owner * rows + r * part_rows
        return pl.ds(pl.multiple_of(start, part_rows), part_rows)

    def half(j, h, r, owner):
        part = grad.at[j, rows_of(owner, r), pl.ds(h * wide, wide)]
        return remote(part, part, half_send.at[j, h, r], half_recv.at[j, h, r], partner)

    def root_part(n, side):
        part = roots.at[side, n * tile :, n * tile : (n + 1) * tile]
        return remote(part, part, root_send.at[n], root_recv.at[n], partner)

    barrier = pltpu.get_barrier_semaphore()
    pl.semaphore_signal(
        barrier, inc=1, device_id={"tok": partner}, device_id_type=pl.DeviceIdType.MESH
    )
    pl.semaphore_signal(
        barrier, inc=1, device_id={"tok": near_device}, device_id_type=pl.DeviceIdType.MESH
    )

    @pl.when(inner)
    def _():
        pl.semaphore_signal(
            barrier, inc=1, device_id={"tok": across_device}, device_id_type=pl.DeviceIdType.MESH
        )

    for r in range(HALVES):
        tok_local(0, r).start()
        if r == 0:
            grad_local(0, 0).start()
    for h in range(1, PIECES):
        grad_local(0, h).start()
    pl.semaphore_wait(barrier, jnp.where(inner, 3, 2))
    for r in range(HALVES):
        tok_remote(0, r).start()
        if r == 0:
            grad_remote(0, 0).start()
    for h in range(1, PIECES):
        grad_remote(0, h).start()

    def wait_tokens(k, r):
        tok_local(k, r).wait()
        tok_remote(k, r).wait_recv()

    def wait_grads(j, h):
        grad_local(j, h).wait()
        grad_remote(j, h).wait_recv()

    def partial(j, k, h, r):
        return lax.dot_general(
            tok2[k, r], grad2[j, h], (((0,), (0,)), ((), ())), preferred_element_type=f32
        )

    def piece(j, k, h):
        @pl.when(k == 0)
        def _():
            wait_grads(j, h)

        for r in range(HALVES):
            if h == 0:

                @pl.when(j == 0)
                def _():
                    wait_tokens(k, r)

            sent_part = partial(j, k, h, r)

            @pl.when(j > 0)
            def _():
                hop(j - 1, k, h, r).wait_send()

            @pl.when(outer)
            def _():
                sent[k, h, r] = sent_part.astype(bf16)

            @pl.when(inner)
            def _():
                slot = jnp.where(k == 2, SENDS, k)
                arrived(j, slot, h, r)
                sent[k, h, r] = (sent_part + got[j, slot, h, r].astype(f32)).astype(bf16)

            hop(j, k, h, r).start()

    def step(s, carry):
        j, r = s // SENDS, lax.rem(s, SENDS)
        k = jnp.where(outer, r, lax.rem(SENDS - r, SENDS))

        for h in range(PIECES):
            piece(j, k, h)

        @pl.when(s == 0)
        def _():
            for later in range(1, 4):
                for r in range(HALVES):
                    tok_local(later, r).start()
                    tok_remote(later, r).start()

        @pl.when(s == 1)
        def _():
            for later in range(1, blocks):
                for h in range(PIECES):
                    grad_local(later, h).start()
                    grad_remote(later, h).start()
            for later in range(blocks):
                stat_load(later).start()

        return carry

    def put(ref, n, value):
        value = value.astype(bf16)
        ref[n : n + tile, n:] = value
        if n + tile < order:
            ref[n + tile :, n : n + tile] = value[:, tile:].T

    def product(left, right, finish, step=1):
        for n in range(0, order, tile)[::step]:
            total = jnp.dot(left[n : n + tile, :], right[:, n:], preferred_element_type=f32)
            finish(total, n, (slice(n, n + tile), slice(n, None)))

    def one_block(j, carry):
        stat = stats.at[j]
        last = j == blocks - 1
        split = blocks * SENDS
        first = jnp.where(outer, jnp.where(j == 0, 0, split), j * SENDS + jnp.minimum(j, 1))
        end = jnp.where(outer, split, (j + 1) * SENDS)
        lax.fori_loop(first, end, step, 0)

        @pl.when(j == 0)
        def _():
            for r in range(HALVES):
                wait_tokens(SENDS, r)

        def ahead(h):
            @pl.when(jnp.logical_and(inner, jnp.logical_not(last)))
            def _():
                piece(j + 1, 0, h)

        for h in range(PIECES):
            for r in range(HALVES):
                own32[h, r] = partial(j, SENDS, h, r)
        stat_load(j).wait()

        def norm(total, own, other):
            square = jnp.sum(total * total, axis=0, keepdims=True)
            value = jnp.sum(square[:, own], axis=1, keepdims=True)
            if other is not None:
                value = value + 2.0 * jnp.sum(square[:, other], axis=1, keepdims=True)
            return value

        def gram_left(h):
            columns = slice(h * wide, (h + 1) * wide)
            sums = jnp.zeros((1, 1), f32)
            for n in range(0, order, tile):
                at = (slice(n, n + tile), slice(n, None))
                total = stat[at] + lax.dot_general(
                    grad[j, n : n + tile, columns], grad[j, n:, columns],
                    (((1,), (1,)), ((), ())), preferred_element_type=f32,
                )
                stat[at] = total
                if h == PIECES - 1:
                    put(scaled, n, total)
                    rest = slice(tile, None) if n + tile < order else None
                    sums = sums + norm(total, slice(0, tile), rest)
            if h == PIECES - 1:
                own32[0, 0, 0:1, 0:wide] = jnp.broadcast_to(sums, (1, wide))

        def gram_right(h):
            n, reach = h * tile, (h + 1) * tile
            total = stat[:reach, n:reach] + lax.dot_general(
                grad[j, :, :reach], grad[j, :, n:reach], (((0,), (0,)), ((), ())),
                preferred_element_type=f32,
            )
            stat[:reach, n:reach] = total
            scaled[:reach, n:reach] = total.astype(bf16)
            diagonal = total[n:]
            sums = jnp.sum(jnp.sum(diagonal * diagonal, axis=0, keepdims=True), axis=1, keepdims=True)
            if h:
                above = total[:n]
                scaled[n:reach, :n] = above.astype(bf16).T
                sums = sums + 2.0 * jnp.sum(
                    jnp.sum(above * above, axis=0, keepdims=True), axis=1, keepdims=True
                )
                sums = sums + own32[0, 0, 0:1, 0:1]
            own32[0, 0, 0:1, 0:wide] = jnp.broadcast_to(sums, (1, wide))

        for h in range(PIECES):
            for r in range(HALVES):
                arrived(j, 2, h, r)

                @pl.when(outer)
                def _():
                    own32[h, r] = own32[h, r] + got[j, 2, h, r].astype(f32)

                @pl.when(inner)
                def _():
                    arrived(j, SENDS + 1, h, r)
                    own32[h, r] = (
                        own32[h, r]
                        + got[j, 2, h, r].astype(f32)
                        + got[j, SENDS + 1, h, r].astype(f32)
                    )

                grad[j, rows_of(core, r), h * wide : (h + 1) * wide] = own32[h, r].astype(bf16)
                half(j, h, r, core).start()
            for r in range(HALVES):
                half(j, h, r, 1 - core).wait_recv()
            pl.when(core == 0)(functools.partial(gram_left, h))
            pl.when(core == 1)(functools.partial(gram_right, h))

        zeta = 2.5 / jnp.sqrt(own32[0, 0, 0:1, 0:1] + 1e-06)
        gain = jnp.sqrt(jnp.sqrt(zeta))

        def first_square(total, n, at):
            put(one, n, (zeta * zeta * 0.0625) * total - (0.625 * zeta) * stat[at])
            if n + tile < order:
                stat[n + tile :, n : n + tile] = stat[n : n + tile, n + tile :].T

        product(scaled, scaled, first_square)
        ahead(0)

        def first_fourth(total, n, at):
            put(two, n, 3.125 * one[at].astype(f32) + total)

        product(one, one, first_fourth)

        def second(total, n, at):
            put(three, n, zeta * (2.44140625 * stat[at] + total))

        product(two, scaled, second)
        ahead(1)

        def second_square(total, n, at):
            base = three[at].astype(f32)
            put(one, n, (total - 10.0 * base) * 0.0625)
            put(two, n, (5.0 * base - total) * 0.25)

        product(three, three, second_square)
        mine = roots.at[core]

        def second_fourth(total, n, at):
            put(mine, n, 3.125 * one[at].astype(f32) + total)

        product(one, one, second_fourth)
        ahead(2)

        def factors(total, n, at):
            value = -0.25 * (
                1.25 * three[at].astype(f32) + 2.44140625 * two[at].astype(f32) + total
            )
            put(one, n, value)
            three[at] = (value - value.astype(bf16).astype(f32)).astype(bf16)

        product(mine, two, factors)

        def final(total, n, at):
            shape = total.shape
            unit = (
                lax.broadcasted_iota(jnp.int32, shape, 0)
                == lax.broadcasted_iota(jnp.int32, shape, 1)
            ).astype(f32)
            rest = one[at].astype(f32) + three[at].astype(f32)
            value = 1.953125 * unit + 1.25 * rest - zeta * (0.390625 * stat[at] + 0.25 * total)
            put(mine, n, gain * value)
            root_part(n // tile, core).start()

        product(one, scaled, final, -1)
        ahead(3)

        def roots_arrived():
            theirs = roots.at[1 - core]
            for n in range(PIECES)[::-1]:
                root_part(n, 1 - core).wait_recv()
                first, past = n * tile, (n + 1) * tile
                if past < order:
                    theirs[first:past, past:] = theirs[past:, first:past].T

        pl.when(jnp.logical_or(core == 1, last))(roots_arrived)

        @pl.when(jnp.logical_not(last))
        def _():
            left = roots[0, pl.ds(pl.multiple_of(core * rows, rows), rows), :]
            three[:rows] = jnp.dot(left, grad[j], preferred_element_type=f32).astype(bf16)
            pl.when(core == 0)(roots_arrived)
            staged[j] = (
                jnp.dot(three[:rows], roots[1], preferred_element_type=f32) * math.sqrt(order)
            ).astype(bf16)

        for n in range(PIECES):
            root_part(n, core).wait_send()
        return carry

    lax.fori_loop(0, blocks, one_block, 0)
    for h in range(PIECES):
        for j in range(blocks):
            grad_remote(j, h).wait_send()
    for r in range(HALVES):
        for k in range(4):
            tok_remote(k, r).wait_send()
        for h in range(PIECES):
            for j in range(blocks):
                half(j, h, r, core).wait_send()
            for k in range(SENDS):
                hop(blocks - 1, k, h, r).wait_send()


def last_kernel(blocks, stats, roots, grad, staged, update, fresh, mixed, final, sems):
    f32, bf16 = jnp.float32, jnp.bfloat16
    order = grad.shape[1]
    rows = order // 2
    core = lax.rem(lax.axis_index("tok"), 2)
    copies = [
        pltpu.make_async_copy(stats.at[j], fresh.at[j, 0], sems.at[j]) for j in range(blocks)
    ]
    copies += [
        pltpu.make_async_copy(
            staged.at[j], update.at[:, j * order : (j + 1) * order], sems.at[blocks + j]
        )
        for j in range(blocks - 1)
    ]
    for copy in copies:
        copy.start()
    left = roots[0, pl.ds(pl.multiple_of(core * rows, rows), rows), :]
    mixed[...] = jnp.dot(left, grad[blocks - 1], preferred_element_type=f32).astype(bf16)
    for h in range(2):
        half = slice(h * (rows // 2), (h + 1) * (rows // 2))
        final[half] = (
            jnp.dot(mixed[half], roots[1], preferred_element_type=f32) * math.sqrt(order)
        ).astype(bf16)
        copy = pltpu.make_async_copy(
            final.at[half], update.at[half, (blocks - 1) * order :], sems.at[2 * blocks - 1 + h]
        )
        copy.start()
        copies.append(copy)
    for copy in copies:
        copy.wait()


def on_device(tokens, grads_out, statistics):
    blocks, _, order, piece_width = statistics.shape
    count = lax.axis_size("tok")
    if piece_width != order or count != 2 * LINE or tokens.shape[1] != LINE * order:
        return in_pieces(tokens, grads_out, statistics)
    local, rows, wide = tokens.shape[0], order // 2, order // PIECES
    part = rows // HALVES
    bf16, f32 = jnp.bfloat16, jnp.float32
    dma = pltpu.SemaphoreType.DMA
    anywhere = pl.BlockSpec(memory_space=pl.ANY)
    near = pl.BlockSpec(memory_space=pltpu.VMEM)
    square = pltpu.VMEM((order, order), bf16)
    held = pl.pallas_call(
        functools.partial(fused_kernel, blocks),
        out_shape=(
            pltpu.VMEM((blocks, order, order), f32),
            pltpu.VMEM((2, order, order), bf16),
            pltpu.VMEM((blocks, order, order), bf16),
            pltpu.VMEM((max(blocks - 1, 1), rows, order), bf16),
        ),
        in_specs=[anywhere] * 3,
        out_specs=(near,) * 4,
        scratch_shapes=[
            pltpu.VMEM((4, HALVES, 2 * local, part), bf16),
            pltpu.VMEM((blocks, PIECES, 2 * local, wide), bf16),
            pltpu.VMEM((SENDS, PIECES, HALVES, part, wide), bf16),
            pltpu.VMEM((blocks, SLOTS, PIECES, HALVES, part, wide), bf16),
            pltpu.VMEM((PIECES, HALVES, part, wide), f32),
            square,
            square,
            square,
            square,
            dma((4, HALVES)),
            dma((4, HALVES)),
            dma((4, HALVES)),
            dma((blocks, PIECES)),
            dma((blocks, PIECES)),
            dma((blocks, PIECES)),
            dma((SENDS, PIECES, HALVES)),
            dma((blocks, SLOTS, PIECES, HALVES)),
            dma((blocks, PIECES, HALVES)),
            dma((blocks, PIECES, HALVES)),
            dma((blocks,)),
            dma((PIECES,)),
            dma((PIECES,)),
        ],
        compiler_params=pltpu.CompilerParams(
            collective_id=0, has_side_effects=True, vmem_limit_bytes=46 << 20
        ),
    )(tokens, grads_out, statistics)
    return pl.pallas_call(
        functools.partial(last_kernel, blocks),
        out_shape=(
            jax.ShapeDtypeStruct((rows, blocks * order), bf16),
            jax.ShapeDtypeStruct(statistics.shape, f32),
        ),
        in_specs=[near] * 4,
        out_specs=(anywhere, anywhere),
        scratch_shapes=[
            pltpu.VMEM((rows, order), bf16),
            pltpu.VMEM((rows, order), bf16),
            dma((2 * blocks + 1,)),
        ],
        compiler_params=pltpu.CompilerParams(vmem_limit_bytes=24 << 20),
    )(*held)


def solution(mesh):
    placed = (P("tok", None), P("tok", "col"), P("col", "tok", None, None))
    return jax.shard_map(
        on_device,
        mesh=mesh,
        in_specs=placed,
        out_specs=(P("tok", "col"), P("col", "tok", None, None)),
        check_vma=False,
    )
```

```python
import functools
import math

import jax
import jax.numpy as jnp
from jax import lax
from jax.experimental import pallas as pl
from jax.experimental.pallas import tpu as pltpu
from jax.sharding import PartitionSpec as P

ITERS = 3


def swapped(block, axis, bit):
    count = lax.axis_size(axis)
    route = []
    for low in range(count):
        high = low | 1 << bit
        if high != low and high < count:
            route += [(low, high), (high, low)]
    return lax.ppermute(block, axis, route)


def as_sent(array):
    return jax.tree.map(lambda a: a.astype(jnp.bfloat16) if a.dtype == jnp.float32 else a, array)


def doubling(values, levels, device, axis_dim, partner):
    for level_bit in range(levels):
        partner_part = partner(values, level_bit)
        low_side = device // 2**level_bit % 2 == 0
        values = jnp.where(
            low_side,
            jnp.concatenate([values, partner_part], axis_dim),
            jnp.concatenate([partner_part, values], axis_dim),
        )
    return values


def product(left_side, right_side):
    return jnp.einsum("bij,bjk->bik", left_side, right_side, precision=lax.Precision.HIGHEST)


def in_pieces(tokens, grads_out, statistics):
    device = lax.axis_index("tok")
    blocks = statistics.shape[0]
    order_size = statistics.shape[2]
    piece_width = statistics.shape[3]
    pieces = order_size // piece_width
    levels = pieces.bit_length() - 1
    rows_dev = tokens.shape[1] // lax.axis_size("tok")
    side_bit = device // pieces % 2
    column = device % pieces
    slab_index = device % (2 * pieces)

    def columns_of(values):
        return lax.dynamic_slice_in_dim(values, column * piece_width, piece_width, 2)

    owned = lax.psum_scatter(
        lax.dot_general(
            tokens, grads_out, (((0,), (0,)), ((), ())), preferred_element_type=jnp.float32
        ),
        "tok",
        scatter_dimension=0,
        tiled=True,
    ).astype(jnp.bfloat16)
    gradient = doubling(
        owned, levels + 1, device, 0, lambda portion, level_bit: swapped(portion, "tok", level_bit)
    )
    grad_cube = gradient.reshape(order_size, blocks, order_size)
    forward = jnp.transpose(grad_cube, (1, 0, 2))
    backward = jnp.transpose(grad_cube, (1, 2, 0))
    oriented = jnp.where(side_bit == 0, forward, backward)
    own_rows = lax.dynamic_slice_in_dim(oriented, column * piece_width, piece_width, 1)
    gram_piece = jnp.einsum("brc,bqc->brq", oriented, own_rows, preferred_element_type=jnp.float32)
    fresh_stat = statistics[:, 0] + gram_piece
    identity = jnp.eye(order_size, dtype=jnp.float32)

    def widen(values):
        return doubling(
            values, levels, device, 2, lambda portion, level_bit: swapped(portion, "tok", level_bit)
        )

    assembled = widen(fresh_stat)
    scaling = (2.5 / jnp.sqrt(jnp.sum(assembled * assembled, axis=(1, 2)) + 1e-06))[:, None, None]
    matrix = scaling * assembled
    factor = (5.0 * identity - matrix) * 0.25
    iterate = jnp.sqrt(jnp.sqrt(scaling)) * columns_of(factor)
    for repeat in range(1, ITERS):
        square = widen(product(factor, columns_of(factor)))
        fourth = widen(product(square, columns_of(square)))
        matrix = widen(product(fourth, columns_of(matrix)))
        factor = (5.0 * identity - matrix) * 0.25
        iterate = product(factor, iterate)
    own_root = doubling(
        iterate.astype(jnp.bfloat16),
        levels,
        device,
        2,
        lambda portion, level_bit: jax.tree.map(
            lambda part, own: part.astype(own.dtype),
            swapped(as_sent(portion), "tok", level_bit),
            portion,
        ),
    )
    other_root = swapped(own_root, "tok", levels)
    left_root = jnp.where(side_bit == 0, own_root, other_root)
    right_root = jnp.where(side_bit == 0, other_root, own_root)
    left_rows = lax.dynamic_slice_in_dim(left_root, slab_index * rows_dev, rows_dev, 1)
    mixed_rows = jnp.einsum(
        "bsr,rbc->bsc", left_rows, grad_cube, preferred_element_type=jnp.float32
    ).astype(jnp.bfloat16)
    update = jnp.einsum(
        "bsc,bcd->sbd", mixed_rows, right_root, preferred_element_type=jnp.float32
    ) * math.sqrt(order_size)
    return (update.reshape(rows_dev, blocks * order_size).astype(jnp.bfloat16), fresh_stat[:, None])


LINE = 4
SENDS = 3
SLOTS = 5
PIECES = 4
HALVES = 2


def fused_kernel(
    blocks, tokens, grads, old, stats, roots, grad, staged,
    tok2, grad2, sent, got, own32, scaled, one, two, three,
    tok_in, tok_send, tok_recv, grad_in, grad_send, grad_recv, hop_send, hop_recv,
    half_send, half_recv, stat_in, root_send, root_recv,
):
    f32, bf16 = jnp.float32, jnp.bfloat16
    order = grad.shape[1]
    local = tokens.shape[0]
    rows = order // 2
    part_rows = rows // HALVES
    wide = tile = order // PIECES
    me = lax.axis_index("tok")
    spot, core = me // 2, lax.rem(me, 2)
    partner = spot * 2 + 1 - core
    outer = jnp.logical_or(spot == 0, spot == LINE - 1)
    inner = jnp.logical_not(outer)
    low = spot < LINE // 2
    near = spot + 1 - 2 * lax.rem(spot, 2)
    across = LINE - 1 - spot
    near_device, across_device = near * 2 + core, across * 2 + core

    def chunk_of(k):
        far = jnp.where(low, LINE - 1 - k, k)
        return jnp.where(k < 2, far, jnp.where(k == 2, near, spot))

    def remote(source, target, send, recv, device):
        return pltpu.make_async_remote_copy(
            src_ref=source, dst_ref=target, send_sem=send, recv_sem=recv,
            device_id={"tok": device}, device_id_type=pl.DeviceIdType.MESH,
        )

    def columns(k, r, owner):
        start = (chunk_of(k) * 2 + owner) * rows + r * part_rows
        return pl.ds(pl.multiple_of(start, part_rows), part_rows)

    def tok_local(k, r):
        return pltpu.make_async_copy(
            tokens.at[:, columns(k, r, core)], tok2.at[k, r, pl.ds(0, local), :], tok_in.at[k, r]
        )

    def tok_remote(k, r):
        return remote(
            tokens.at[:, columns(k, r, 1 - core)], tok2.at[k, r, pl.ds(local, local), :],
            tok_send.at[k, r], tok_recv.at[k, r], partner,
        )

    def grad_columns(j, h):
        return pl.ds(pl.multiple_of(j * order + h * wide, wide), wide)

    def grad_local(j, h):
        return pltpu.make_async_copy(
            grads.at[:, grad_columns(j, h)], grad2.at[j, h, pl.ds(0, local), :], grad_in.at[j, h]
        )

    def grad_remote(j, h):
        return remote(
            grads.at[:, grad_columns(j, h)], grad2.at[j, h, pl.ds(local, local), :],
            grad_send.at[j, h], grad_recv.at[j, h], partner,
        )

    def stat_load(j):
        return pltpu.make_async_copy(old.at[j, 0], stats.at[j], stat_in.at[j])

    def hop(j, k, h, r):
        slot = jnp.where(jnp.logical_or(outer, k == 2), k, SENDS + k)
        device = jnp.where(jnp.logical_or(outer, k == 2), near_device, across_device)
        return remote(
            sent.at[k, h, r], got.at[j, slot, h, r], hop_send.at[k, h, r],
            hop_recv.at[j, slot, h, r], device,
        )

    def arrived(j, slot, h, r):
        remote(
            sent.at[0, h, r], got.at[j, slot, h, r], hop_send.at[0, h, r],
            hop_recv.at[j, slot, h, r], near_device,
        ).wait_recv()

    def rows_of(owner, r):
        start = owner * rows + r * part_rows
        return pl.ds(pl.multiple_of(start, part_rows), part_rows)

    def half(j, h, r, owner):
        part = grad.at[j, rows_of(owner, r), pl.ds(h * wide, wide)]
        return remote(part, part, half_send.at[j, h, r], half_recv.at[j, h, r], partner)

    def root_part(n, side):
        if n == PIECES:
            part = roots.at[side, :rows, :tile]
        else:
            part = roots.at[side, n * tile if n else rows :, n * tile : (n + 1) * tile]
        return remote(part, part, root_send.at[n], root_recv.at[n], partner)

    barrier = pltpu.get_barrier_semaphore()
    pl.semaphore_signal(
        barrier, inc=1, device_id={"tok": partner}, device_id_type=pl.DeviceIdType.MESH
    )
    pl.semaphore_signal(
        barrier, inc=1, device_id={"tok": near_device}, device_id_type=pl.DeviceIdType.MESH
    )

    @pl.when(inner)
    def _():
        pl.semaphore_signal(
            barrier, inc=1, device_id={"tok": across_device}, device_id_type=pl.DeviceIdType.MESH
        )

    for r in range(HALVES):
        tok_local(0, r).start()
        if r == 0:
            grad_local(0, 0).start()
    for h in range(1, PIECES):
        grad_local(0, h).start()
    pl.semaphore_wait(barrier, jnp.where(inner, 3, 2))
    for r in range(HALVES):
        tok_remote(0, r).start()
        if r == 0:
            grad_remote(0, 0).start()
    for h in range(1, PIECES):
        grad_remote(0, h).start()

    def partial(j, k, h, r, rows=slice(None)):
        return lax.dot_general(
            tok2[k, r, rows], grad2[j, h, rows], (((0,), (0,)), ((), ())),
            preferred_element_type=f32,
        )

    def piece(j, k, h):
        pl.when(k == 0)(lambda: grad_local(j, h).wait())
        if h:
            pl.when(k == 0)(lambda: grad_remote(j, h).wait_recv())
        for r in range(HALVES):
            if h == 0:
                pl.when(j == 0)(lambda: tok_local(k, r).wait())
                sent_part = partial(j, k, h, r, slice(0, local))
                if r == 0:
                    pl.when(k == 0)(lambda: grad_remote(j, h).wait_recv())
                pl.when(j == 0)(lambda: tok_remote(k, r).wait_recv())
                sent_part = sent_part + partial(j, k, h, r, slice(local, 2 * local))
            else:
                sent_part = partial(j, k, h, r)

            @pl.when(j > 0)
            def _():
                hop(j - 1, k, h, r).wait_send()

            @pl.when(outer)
            def _():
                sent[k, h, r] = sent_part.astype(bf16)

            @pl.when(inner)
            def _():
                slot = jnp.where(k == 2, SENDS, k)
                arrived(j, slot, h, r)
                sent[k, h, r] = (sent_part + got[j, slot, h, r].astype(f32)).astype(bf16)

            hop(j, k, h, r).start()

    def step(s, carry):
        j, r = s // SENDS, lax.rem(s, SENDS)
        k = jnp.where(outer, r, lax.rem(SENDS - r, SENDS))

        for h in range(PIECES):
            piece(j, k, h)

        @pl.when(s == 0)
        def _():
            for later in range(1, 4):
                for r in range(HALVES):
                    tok_local(later, r).start()
                    tok_remote(later, r).start()

        @pl.when(s == 1)
        def _():
            for later in range(1, blocks):
                for h in range(PIECES):
                    grad_local(later, h).start()
                    grad_remote(later, h).start()
            for later in range(blocks):
                stat_load(later).start()

        return carry

    def put(ref, n, value):
        value = value.astype(bf16)
        ref[n : n + tile, n:] = value
        if n + tile < order:
            ref[n + tile :, n : n + tile] = value[:, tile:].T

    def product(left, right, finish, step=1, first=0):
        for n in range(first * tile, order, tile)[::step]:
            total = jnp.dot(left[n : n + tile, :], right[:, n:], preferred_element_type=f32)
            finish(total, n, (slice(n, n + tile), slice(n, None)))

    def one_block(j, carry):
        stat = stats.at[j]
        last = j == blocks - 1
        split = blocks * SENDS
        first = jnp.where(outer, jnp.where(j == 0, 0, split), j * SENDS + jnp.minimum(j, 1))
        end = jnp.where(outer, split, (j + 1) * SENDS)
        lax.fori_loop(first, end, step, 0)

        @pl.when(j == 0)
        def _():
            for r in range(HALVES):
                tok_local(SENDS, r).wait()
                tok_remote(SENDS, r).wait_recv()

        def ahead(h):
            @pl.when(jnp.logical_and(inner, jnp.logical_not(last)))
            def _():
                piece(j + 1, 0, h)

        for h in range(PIECES):
            for r in range(HALVES):
                own32[h, r] = partial(j, SENDS, h, r)
        stat_load(j).wait()

        def norm(total, own, other):
            square = jnp.sum(total * total, axis=0, keepdims=True)
            value = jnp.sum(square[:, own], axis=1, keepdims=True)
            if other is not None:
                value = value + 2.0 * jnp.sum(square[:, other], axis=1, keepdims=True)
            return value

        def gram_left(h):
            columns = slice(h * wide, (h + 1) * wide)
            sums = jnp.zeros((1, 1), f32)
            for n in range(0, order, tile):
                at = (slice(n, n + tile), slice(n, None))
                total = stat[at] + lax.dot_general(
                    grad[j, n : n + tile, columns], grad[j, n:, columns],
                    (((1,), (1,)), ((), ())), preferred_element_type=f32,
                )
                stat[at] = total
                if h == PIECES - 1:
                    put(scaled, n, total)
                    rest = slice(tile, None) if n + tile < order else None
                    sums = sums + norm(total, slice(0, tile), rest)
            if h == PIECES - 1:
                own32[0, 0, 0:1, 0:wide] = jnp.broadcast_to(sums, (1, wide))

        def gram_right(h):
            n, reach = h * tile, (h + 1) * tile
            total = stat[:reach, n:reach] + lax.dot_general(
                grad[j, :, :reach], grad[j, :, n:reach], (((0,), (0,)), ((), ())),
                preferred_element_type=f32,
            )
            stat[:reach, n:reach] = total
            scaled[:reach, n:reach] = total.astype(bf16)
            diagonal = total[n:]
            sums = jnp.sum(jnp.sum(diagonal * diagonal, axis=0, keepdims=True), axis=1, keepdims=True)
            if h:
                above = total[:n]
                scaled[n:reach, :n] = above.astype(bf16).T
                sums = sums + 2.0 * jnp.sum(
                    jnp.sum(above * above, axis=0, keepdims=True), axis=1, keepdims=True
                )
                sums = sums + own32[0, 0, 0:1, 0:1]
            own32[0, 0, 0:1, 0:wide] = jnp.broadcast_to(sums, (1, wide))

        for h in range(PIECES):
            for r in range(HALVES):
                arrived(j, 2, h, r)

                @pl.when(outer)
                def _():
                    own32[h, r] = own32[h, r] + got[j, 2, h, r].astype(f32)

                @pl.when(inner)
                def _():
                    arrived(j, SENDS + 1, h, r)
                    own32[h, r] = (
                        own32[h, r]
                        + got[j, 2, h, r].astype(f32)
                        + got[j, SENDS + 1, h, r].astype(f32)
                    )

                grad[j, rows_of(core, r), h * wide : (h + 1) * wide] = own32[h, r].astype(bf16)
                half(j, h, r, core).start()
            for r in range(HALVES):
                half(j, h, r, 1 - core).wait_recv()
            pl.when(core == 0)(functools.partial(gram_left, h))
            pl.when(core == 1)(functools.partial(gram_right, h))

        zeta = 2.5 / jnp.sqrt(own32[0, 0, 0:1, 0:1] + 1e-06)
        gain = jnp.sqrt(jnp.sqrt(zeta))

        def lower_half(n):
            if n + tile < order:
                stat[n + tile :, n : n + tile] = stat[n : n + tile, n + tile :].T

        def first_square(total, n, at):
            put(one, n, (zeta * zeta * 0.0625) * total - (0.625 * zeta) * stat[at])
            if n:
                lower_half(n)

        product(scaled, scaled, first_square)

        def first_fourth(total, n, at):
            put(two, n, 3.125 * one[at].astype(f32) + total)
            if n == 0:
                lower_half(n)

        product(one, one, first_fourth)

        def second(total, n, at):
            put(three, n, zeta * (2.44140625 * stat[at] + total))

        product(two, scaled, second)

        def second_square(total, n, at):
            base = three[at].astype(f32)
            put(one, n, (total - 10.0 * base) * 0.0625)
            put(two, n, (5.0 * base - total) * 0.25)

        product(three, three, second_square)
        mine = roots.at[core]

        def second_fourth(total, n, at):
            put(mine, n, 3.125 * one[at].astype(f32) + total)

        product(one, one, second_fourth)
        ahead(0)
        ahead(1)

        def factors(total, n, at):
            value = -0.25 * (
                1.25 * three[at].astype(f32) + 2.44140625 * two[at].astype(f32) + total
            )
            put(one, n, value)
            three[at] = (value - value.astype(bf16).astype(f32)).astype(bf16)

        product(mine, two, factors)

        def final(total, n, at):
            shape = total.shape
            unit = (
                lax.broadcasted_iota(jnp.int32, shape, 0) + n
                == lax.broadcasted_iota(jnp.int32, shape, 1) + at[1].start
            ).astype(f32)
            rest = one[at].astype(f32) + three[at].astype(f32)
            value = 1.953125 * unit + 1.25 * rest - zeta * (0.390625 * stat[at] + 0.25 * total)
            return gain * value

        def final_rows(total, n, at):
            put(mine, n, final(total, n, at))
            root_part(n // tile, core).start()

        def final_first(start, end):
            at = (slice(0, tile), slice(start, end))
            total = jnp.dot(one[:tile, :], scaled[:, start:end], preferred_element_type=f32)
            value = final(total, 0, at).astype(bf16)
            mine[at] = value
            skip = 0 if start else tile
            mine[start + skip : end, :tile] = value[:, skip:].T

        product(one, scaled, final_rows, -1, 1)
        final_first(rows, order)
        root_part(0, core).start()
        final_first(0, rows)
        root_part(PIECES, core).start()
        ahead(2)
        ahead(3)

        def roots_arrived():
            theirs = roots.at[1 - core]
            for n in range(PIECES)[::-1]:
                root_part(n, 1 - core).wait_recv()
                if n == 0:
                    theirs[:tile, rows:] = theirs[rows:, :tile].T
                    root_part(PIECES, 1 - core).wait_recv()
                    theirs[:tile, tile:rows] = theirs[tile:rows, :tile].T
                    break
                first, past = n * tile, (n + 1) * tile
                if past < order:
                    theirs[first:past, past:] = theirs[past:, first:past].T

        pl.when(jnp.logical_or(core == 1, last))(roots_arrived)

        @pl.when(jnp.logical_not(last))
        def _():
            left = roots[0, pl.ds(pl.multiple_of(core * rows, rows), rows), :]
            three[:rows] = jnp.dot(left, grad[j], preferred_element_type=f32).astype(bf16)
            pl.when(core == 0)(roots_arrived)
            staged[j] = (
                jnp.dot(three[:rows], roots[1], preferred_element_type=f32) * math.sqrt(order)
            ).astype(bf16)

        for n in range(PIECES + 1):
            root_part(n, core).wait_send()
        return carry

    lax.fori_loop(0, blocks, one_block, 0)
    for h in range(PIECES):
        for j in range(blocks):
            grad_remote(j, h).wait_send()
    for r in range(HALVES):
        for k in range(4):
            tok_remote(k, r).wait_send()
        for h in range(PIECES):
            for j in range(blocks):
                half(j, h, r, core).wait_send()
            for k in range(SENDS):
                hop(blocks - 1, k, h, r).wait_send()


def last_kernel(blocks, stats, roots, grad, staged, update, fresh, mixed, final, sems):
    f32, bf16 = jnp.float32, jnp.bfloat16
    order = grad.shape[1]
    rows = order // 2
    core = lax.rem(lax.axis_index("tok"), 2)
    copies = [
        pltpu.make_async_copy(stats.at[j], fresh.at[j, 0], sems.at[j]) for j in range(blocks)
    ]
    copies += [
        pltpu.make_async_copy(
            staged.at[j], update.at[:, j * order : (j + 1) * order], sems.at[blocks + j]
        )
        for j in range(blocks - 1)
    ]
    for copy in copies:
        copy.start()
    left = roots[0, pl.ds(pl.multiple_of(core * rows, rows), rows), :]
    mixed[...] = jnp.dot(left, grad[blocks - 1], preferred_element_type=f32).astype(bf16)
    for h in range(2):
        half = slice(h * (rows // 2), (h + 1) * (rows // 2))
        final[half] = (
            jnp.dot(mixed[half], roots[1], preferred_element_type=f32) * math.sqrt(order)
        ).astype(bf16)
        copy = pltpu.make_async_copy(
            final.at[half], update.at[half, (blocks - 1) * order :], sems.at[2 * blocks - 1 + h]
        )
        copy.start()
        copies.append(copy)
    for copy in copies:
        copy.wait()


def on_device(tokens, grads_out, statistics):
    blocks, _, order, piece_width = statistics.shape
    count = lax.axis_size("tok")
    if piece_width != order or count != 2 * LINE or tokens.shape[1] != LINE * order:
        return in_pieces(tokens, grads_out, statistics)
    local, rows, wide = tokens.shape[0], order // 2, order // PIECES
    part = rows // HALVES
    bf16, f32 = jnp.bfloat16, jnp.float32
    dma = pltpu.SemaphoreType.DMA
    anywhere = pl.BlockSpec(memory_space=pl.ANY)
    near = pl.BlockSpec(memory_space=pltpu.VMEM)
    square = pltpu.VMEM((order, order), bf16)
    held = pl.pallas_call(
        functools.partial(fused_kernel, blocks),
        out_shape=(
            pltpu.VMEM((blocks, order, order), f32),
            pltpu.VMEM((2, order, order), bf16),
            pltpu.VMEM((blocks, order, order), bf16),
            pltpu.VMEM((max(blocks - 1, 1), rows, order), bf16),
        ),
        in_specs=[anywhere] * 3,
        out_specs=(near,) * 4,
        scratch_shapes=[
            pltpu.VMEM((4, HALVES, 2 * local, part), bf16),
            pltpu.VMEM((blocks, PIECES, 2 * local, wide), bf16),
            pltpu.VMEM((SENDS, PIECES, HALVES, part, wide), bf16),
            pltpu.VMEM((blocks, SLOTS, PIECES, HALVES, part, wide), bf16),
            pltpu.VMEM((PIECES, HALVES, part, wide), f32),
            square,
            square,
            square,
            square,
            dma((4, HALVES)),
            dma((4, HALVES)),
            dma((4, HALVES)),
            dma((blocks, PIECES)),
            dma((blocks, PIECES)),
            dma((blocks, PIECES)),
            dma((SENDS, PIECES, HALVES)),
            dma((blocks, SLOTS, PIECES, HALVES)),
            dma((blocks, PIECES, HALVES)),
            dma((blocks, PIECES, HALVES)),
            dma((blocks,)),
            dma((PIECES + 1,)),
            dma((PIECES + 1,)),
        ],
        compiler_params=pltpu.CompilerParams(
            collective_id=0, has_side_effects=True, vmem_limit_bytes=46 << 20
        ),
    )(tokens, grads_out, statistics)
    return pl.pallas_call(
        functools.partial(last_kernel, blocks),
        out_shape=(
            jax.ShapeDtypeStruct((rows, blocks * order), bf16),
            jax.ShapeDtypeStruct(statistics.shape, f32),
        ),
        in_specs=[near] * 4,
        out_specs=(anywhere, anywhere),
        scratch_shapes=[
            pltpu.VMEM((rows, order), bf16),
            pltpu.VMEM((rows, order), bf16),
            dma((2 * blocks + 1,)),
        ],
        compiler_params=pltpu.CompilerParams(vmem_limit_bytes=24 << 20),
    )(*held)


def solution(mesh):
    placed = (P("tok", None), P("tok", "col"), P("col", "tok", None, None))
    return jax.shard_map(
        on_device,
        mesh=mesh,
        in_specs=placed,
        out_specs=(P("tok", "col"), P("col", "tok", None, None)),
        check_vma=False,
    )
```

```python
import functools
import math

import jax
import jax.numpy as jnp
from jax import lax
from jax.experimental import pallas as pl
from jax.experimental.pallas import tpu as pltpu
from jax.sharding import PartitionSpec as P

ITERS = 3


def swapped(block, axis, bit):
    count = lax.axis_size(axis)
    route = []
    for low in range(count):
        high = low | 1 << bit
        if high != low and high < count:
            route += [(low, high), (high, low)]
    return lax.ppermute(block, axis, route)


def as_sent(array):
    return jax.tree.map(lambda a: a.astype(jnp.bfloat16) if a.dtype == jnp.float32 else a, array)


def doubling(values, levels, device, axis_dim, partner):
    for level_bit in range(levels):
        partner_part = partner(values, level_bit)
        low_side = device // 2**level_bit % 2 == 0
        values = jnp.where(
            low_side,
            jnp.concatenate([values, partner_part], axis_dim),
            jnp.concatenate([partner_part, values], axis_dim),
        )
    return values


def product(left_side, right_side):
    return jnp.einsum("bij,bjk->bik", left_side, right_side, precision=lax.Precision.HIGHEST)


def in_pieces(tokens, grads_out, statistics):
    device = lax.axis_index("tok")
    blocks = statistics.shape[0]
    order_size = statistics.shape[2]
    piece_width = statistics.shape[3]
    pieces = order_size // piece_width
    levels = pieces.bit_length() - 1
    rows_dev = tokens.shape[1] // lax.axis_size("tok")
    side_bit = device // pieces % 2
    column = device % pieces
    slab_index = device % (2 * pieces)

    def columns_of(values):
        return lax.dynamic_slice_in_dim(values, column * piece_width, piece_width, 2)

    owned = lax.psum_scatter(
        lax.dot_general(
            tokens, grads_out, (((0,), (0,)), ((), ())), preferred_element_type=jnp.float32
        ),
        "tok",
        scatter_dimension=0,
        tiled=True,
    ).astype(jnp.bfloat16)
    gradient = doubling(
        owned, levels + 1, device, 0, lambda portion, level_bit: swapped(portion, "tok", level_bit)
    )
    grad_cube = gradient.reshape(order_size, blocks, order_size)
    forward = jnp.transpose(grad_cube, (1, 0, 2))
    backward = jnp.transpose(grad_cube, (1, 2, 0))
    oriented = jnp.where(side_bit == 0, forward, backward)
    own_rows = lax.dynamic_slice_in_dim(oriented, column * piece_width, piece_width, 1)
    gram_piece = jnp.einsum("brc,bqc->brq", oriented, own_rows, preferred_element_type=jnp.float32)
    fresh_stat = statistics[:, 0] + gram_piece
    identity = jnp.eye(order_size, dtype=jnp.float32)

    def widen(values):
        return doubling(
            values, levels, device, 2, lambda portion, level_bit: swapped(portion, "tok", level_bit)
        )

    assembled = widen(fresh_stat)
    scaling = (2.5 / jnp.sqrt(jnp.sum(assembled * assembled, axis=(1, 2)) + 1e-06))[:, None, None]
    matrix = scaling * assembled
    factor = (5.0 * identity - matrix) * 0.25
    iterate = jnp.sqrt(jnp.sqrt(scaling)) * columns_of(factor)
    for repeat in range(1, ITERS):
        square = widen(product(factor, columns_of(factor)))
        fourth = widen(product(square, columns_of(square)))
        matrix = widen(product(fourth, columns_of(matrix)))
        factor = (5.0 * identity - matrix) * 0.25
        iterate = product(factor, iterate)
    own_root = doubling(
        iterate.astype(jnp.bfloat16),
        levels,
        device,
        2,
        lambda portion, level_bit: jax.tree.map(
            lambda part, own: part.astype(own.dtype),
            swapped(as_sent(portion), "tok", level_bit),
            portion,
        ),
    )
    other_root = swapped(own_root, "tok", levels)
    left_root = jnp.where(side_bit == 0, own_root, other_root)
    right_root = jnp.where(side_bit == 0, other_root, own_root)
    left_rows = lax.dynamic_slice_in_dim(left_root, slab_index * rows_dev, rows_dev, 1)
    mixed_rows = jnp.einsum(
        "bsr,rbc->bsc", left_rows, grad_cube, preferred_element_type=jnp.float32
    ).astype(jnp.bfloat16)
    update = jnp.einsum(
        "bsc,bcd->sbd", mixed_rows, right_root, preferred_element_type=jnp.float32
    ) * math.sqrt(order_size)
    return (update.reshape(rows_dev, blocks * order_size).astype(jnp.bfloat16), fresh_stat[:, None])


LINE = 4
SENDS = 3
SLOTS = 5
PIECES = 4
HALVES = 2


def fused_kernel(
    blocks, tokens, grads, old, stats, roots, grad, staged,
    tok2, grad2, sent, got, own32, scaled, one, two, three,
    tok_in, tok_send, tok_recv, grad_in, grad_send, grad_recv, hop_send, hop_recv,
    half_send, half_recv, stat_in, root_send, root_recv,
):
    f32, bf16 = jnp.float32, jnp.bfloat16
    order = grad.shape[1]
    local = tokens.shape[0]
    rows = order // 2
    part_rows = rows // HALVES
    wide = tile = order // PIECES
    me = lax.axis_index("tok")
    spot, core = me // 2, lax.rem(me, 2)
    partner = spot * 2 + 1 - core
    outer = jnp.logical_or(spot == 0, spot == LINE - 1)
    inner = jnp.logical_not(outer)
    low = spot < LINE // 2
    near = spot + 1 - 2 * lax.rem(spot, 2)
    across = LINE - 1 - spot
    near_device, across_device = near * 2 + core, across * 2 + core

    def chunk_of(k):
        far = jnp.where(low, LINE - 1 - k, k)
        return jnp.where(k < 2, far, jnp.where(k == 2, near, spot))

    def remote(source, target, send, recv, device):
        return pltpu.make_async_remote_copy(
            src_ref=source, dst_ref=target, send_sem=send, recv_sem=recv,
            device_id={"tok": device}, device_id_type=pl.DeviceIdType.MESH,
        )

    def columns(k, r, owner):
        start = (chunk_of(k) * 2 + owner) * rows + r * part_rows
        return pl.ds(pl.multiple_of(start, part_rows), part_rows)

    def tok_local(k, r):
        return pltpu.make_async_copy(
            tokens.at[:, columns(k, r, core)], tok2.at[k, r, pl.ds(0, local), :], tok_in.at[k, r]
        )

    def tok_remote(k, r):
        return remote(
            tokens.at[:, columns(k, r, 1 - core)], tok2.at[k, r, pl.ds(local, local), :],
            tok_send.at[k, r], tok_recv.at[k, r], partner,
        )

    def grad_columns(j, h):
        return pl.ds(pl.multiple_of(j * order + h * wide, wide), wide)

    def grad_local(j, h):
        return pltpu.make_async_copy(
            grads.at[:, grad_columns(j, h)], grad2.at[j, h, pl.ds(0, local), :], grad_in.at[j, h]
        )

    def grad_remote(j, h):
        return remote(
            grads.at[:, grad_columns(j, h)], grad2.at[j, h, pl.ds(local, local), :],
            grad_send.at[j, h], grad_recv.at[j, h], partner,
        )

    def stat_load(j):
        return pltpu.make_async_copy(old.at[j, 0], stats.at[j], stat_in.at[j])

    def hop(j, k, h, r):
        slot = jnp.where(jnp.logical_or(outer, k == 2), k, SENDS + k)
        device = jnp.where(jnp.logical_or(outer, k == 2), near_device, across_device)
        return remote(
            sent.at[k, h, r], got.at[j, slot, h, r], hop_send.at[k, h, r],
            hop_recv.at[j, slot, h, r], device,
        )

    def arrived(j, slot, h, r):
        remote(
            sent.at[0, h, r], got.at[j, slot, h, r], hop_send.at[0, h, r],
            hop_recv.at[j, slot, h, r], near_device,
        ).wait_recv()

    def rows_of(owner, r):
        start = owner * rows + r * part_rows
        return pl.ds(pl.multiple_of(start, part_rows), part_rows)

    def half(j, h, r, owner):
        part = grad.at[j, rows_of(owner, r), pl.ds(h * wide, wide)]
        return remote(part, part, half_send.at[j, h, r], half_recv.at[j, h, r], partner)

    def root_part(n, side):
        if n == PIECES:
            part = roots.at[side, :rows, :tile]
        else:
            part = roots.at[side, n * tile if n else rows :, n * tile : (n + 1) * tile]
        return remote(part, part, root_send.at[n], root_recv.at[n], partner)

    barrier = pltpu.get_barrier_semaphore()
    pl.semaphore_signal(
        barrier, inc=1, device_id={"tok": partner}, device_id_type=pl.DeviceIdType.MESH
    )
    pl.semaphore_signal(
        barrier, inc=1, device_id={"tok": near_device}, device_id_type=pl.DeviceIdType.MESH
    )

    @pl.when(inner)
    def _():
        pl.semaphore_signal(
            barrier, inc=1, device_id={"tok": across_device}, device_id_type=pl.DeviceIdType.MESH
        )

    for r in range(HALVES):
        tok_local(0, r).start()
        if r == 0:
            grad_local(0, 0).start()
    for h in range(1, PIECES):
        grad_local(0, h).start()
    pl.semaphore_wait(barrier, jnp.where(inner, 3, 2))
    for r in range(HALVES):
        tok_remote(0, r).start()
        if r == 0:
            grad_remote(0, 0).start()
    for h in range(1, PIECES):
        grad_remote(0, h).start()

    def partial(j, k, h, r, rows=slice(None)):
        return lax.dot_general(
            tok2[k, r, rows], grad2[j, h, rows], (((0,), (0,)), ((), ())),
            preferred_element_type=f32,
        )

    def piece(j, k, h):
        pl.when(k == 0)(lambda: grad_local(j, h).wait())
        if h:
            pl.when(k == 0)(lambda: grad_remote(j, h).wait_recv())
        for r in range(HALVES):
            if h == 0:
                pl.when(j == 0)(lambda: tok_local(k, r).wait())
                sent_part = partial(j, k, h, r, slice(0, local))
                if r == 0:
                    pl.when(k == 0)(lambda: grad_remote(j, h).wait_recv())
                pl.when(j == 0)(lambda: tok_remote(k, r).wait_recv())
                sent_part = sent_part + partial(j, k, h, r, slice(local, 2 * local))
            else:
                sent_part = partial(j, k, h, r)

            @pl.when(j > 0)
            def _():
                hop(j - 1, k, h, r).wait_send()

            @pl.when(outer)
            def _():
                sent[k, h, r] = sent_part.astype(bf16)

            @pl.when(inner)
            def _():
                slot = jnp.where(k == 2, SENDS, k)
                arrived(j, slot, h, r)
                sent[k, h, r] = (sent_part + got[j, slot, h, r].astype(f32)).astype(bf16)

            hop(j, k, h, r).start()

    def step(s, carry):
        j, r = s // SENDS, lax.rem(s, SENDS)
        k = jnp.where(outer, r, lax.rem(SENDS - r, SENDS))

        for h in range(PIECES):
            piece(j, k, h)

        @pl.when(s == 0)
        def _():
            for later in range(1, 4):
                for r in range(HALVES):
                    tok_local(later, r).start()
                    tok_remote(later, r).start()

        @pl.when(s == 1)
        def _():
            for later in range(1, blocks):
                for h in range(PIECES):
                    grad_local(later, h).start()
                    grad_remote(later, h).start()
            for later in range(blocks):
                stat_load(later).start()

        return carry

    def put(ref, n, value):
        value = value.astype(bf16)
        ref[n : n + tile, n:] = value
        if n + tile < order:
            ref[n + tile :, n : n + tile] = value[:, tile:].T

    def product(left, right, finish, step=1, first=0):
        for n in range(first * tile, order, tile)[::step]:
            total = jnp.dot(left[n : n + tile, :], right[:, n:], preferred_element_type=f32)
            finish(total, n, (slice(n, n + tile), slice(n, None)))

    def one_block(j, carry):
        stat = stats.at[j]
        last = j == blocks - 1
        split = blocks * SENDS
        first = jnp.where(outer, jnp.where(j == 0, 0, split), j * SENDS + jnp.minimum(j, 1))
        end = jnp.where(outer, split, (j + 1) * SENDS)
        lax.fori_loop(first, end, step, 0)

        @pl.when(j == 0)
        def _():
            for r in range(HALVES):
                tok_local(SENDS, r).wait()
                tok_remote(SENDS, r).wait_recv()

        def ahead(h):
            @pl.when(jnp.logical_and(inner, jnp.logical_not(last)))
            def _():
                piece(j + 1, 0, h)

        for h in range(PIECES):
            for r in range(HALVES):
                own32[h, r] = partial(j, SENDS, h, r)

        @pl.when(inner)
        def _():
            for h in range(PIECES):
                for r in range(HALVES):
                    arrived(j, SENDS + 1, h, r)
                    own32[h, r] = own32[h, r] + got[j, SENDS + 1, h, r].astype(f32)

        stat_load(j).wait()

        def norm(total, own, other):
            square = jnp.sum(total * total, axis=0, keepdims=True)
            value = jnp.sum(square[:, own], axis=1, keepdims=True)
            if other is not None:
                value = value + 2.0 * jnp.sum(square[:, other], axis=1, keepdims=True)
            return value

        def gram_left(h):
            columns = slice(h * wide, (h + 1) * wide)
            sums = jnp.zeros((1, 1), f32)
            for n in range(0, order, tile):
                at = (slice(n, n + tile), slice(n, None))
                total = stat[at] + lax.dot_general(
                    grad[j, n : n + tile, columns], grad[j, n:, columns],
                    (((1,), (1,)), ((), ())), preferred_element_type=f32,
                )
                stat[at] = total
                if h == PIECES - 1:
                    put(scaled, n, total)
                    rest = slice(tile, None) if n + tile < order else None
                    sums = sums + norm(total, slice(0, tile), rest)
            if h == PIECES - 1:
                own32[0, 0, 0:1, 0:wide] = jnp.broadcast_to(sums, (1, wide))

        def gram_right(h):
            n, reach = h * tile, (h + 1) * tile
            total = stat[:reach, n:reach] + lax.dot_general(
                grad[j, :, :reach], grad[j, :, n:reach], (((0,), (0,)), ((), ())),
                preferred_element_type=f32,
            )
            stat[:reach, n:reach] = total
            scaled[:reach, n:reach] = total.astype(bf16)
            diagonal = total[n:]
            sums = jnp.sum(jnp.sum(diagonal * diagonal, axis=0, keepdims=True), axis=1, keepdims=True)
            if h:
                above = total[:n]
                scaled[n:reach, :n] = above.astype(bf16).T
                sums = sums + 2.0 * jnp.sum(
                    jnp.sum(above * above, axis=0, keepdims=True), axis=1, keepdims=True
                )
                sums = sums + own32[0, 0, 0:1, 0:1]
            own32[0, 0, 0:1, 0:wide] = jnp.broadcast_to(sums, (1, wide))

        for h in range(PIECES):
            for r in range(HALVES):
                arrived(j, 2, h, r)

                total = own32[h, r] + got[j, 2, h, r].astype(f32)
                grad[j, rows_of(core, r), h * wide : (h + 1) * wide] = total.astype(bf16)
                half(j, h, r, core).start()
            for r in range(HALVES):
                half(j, h, r, 1 - core).wait_recv()
            pl.when(core == 0)(functools.partial(gram_left, h))
            pl.when(core == 1)(functools.partial(gram_right, h))

        zeta = 2.5 / jnp.sqrt(own32[0, 0, 0:1, 0:1] + 1e-06)
        gain = jnp.sqrt(jnp.sqrt(zeta))

        def lower_half(n):
            if n + tile < order:
                stat[n + tile :, n : n + tile] = stat[n : n + tile, n + tile :].T

        def first_square(total, n, at):
            put(one, n, (zeta * zeta * 0.0625) * total - (0.625 * zeta) * stat[at])
            if n:
                lower_half(n)

        product(scaled, scaled, first_square)

        def first_fourth(total, n, at):
            put(two, n, 3.125 * one[at].astype(f32) + total)
            if n == 0:
                lower_half(n)

        product(one, one, first_fourth)

        def second(total, n, at):
            put(three, n, zeta * (2.44140625 * stat[at] + total))

        product(two, scaled, second)

        def second_square(total, n, at):
            base = three[at].astype(f32)
            put(one, n, (total - 10.0 * base) * 0.0625)
            put(two, n, (5.0 * base - total) * 0.25)

        product(three, three, second_square)
        mine = roots.at[core]

        def second_fourth(total, n, at):
            put(mine, n, 3.125 * one[at].astype(f32) + total)

        product(one, one, second_fourth)
        ahead(0)
        ahead(1)

        def factors(total, n, at):
            value = -0.25 * (
                1.25 * three[at].astype(f32) + 2.44140625 * two[at].astype(f32) + total
            )
            put(one, n, value)

        product(mine, two, factors)

        def final(total, n, at):
            shape = total.shape
            unit = (
                lax.broadcasted_iota(jnp.int32, shape, 0) + n
                == lax.broadcasted_iota(jnp.int32, shape, 1) + at[1].start
            ).astype(f32)
            rest = one[at].astype(f32)
            value = 1.953125 * unit + 1.25 * rest - zeta * (0.390625 * stat[at] + 0.25 * total)
            return gain * value

        def final_rows(total, n, at):
            put(mine, n, final(total, n, at))
            root_part(n // tile, core).start()

        def final_first(start, end):
            at = (slice(0, tile), slice(start, end))
            total = jnp.dot(one[:tile, :], scaled[:, start:end], preferred_element_type=f32)
            value = final(total, 0, at).astype(bf16)
            mine[at] = value
            skip = 0 if start else tile
            mine[start + skip : end, :tile] = value[:, skip:].T

        product(one, scaled, final_rows, -1, 1)
        final_first(rows, order)
        root_part(0, core).start()
        final_first(0, rows)
        root_part(PIECES, core).start()
        ahead(2)
        ahead(3)

        def roots_arrived():
            theirs = roots.at[1 - core]
            for n in range(PIECES)[::-1]:
                root_part(n, 1 - core).wait_recv()
                if n == 0:
                    theirs[:tile, rows:] = theirs[rows:, :tile].T
                    root_part(PIECES, 1 - core).wait_recv()
                    theirs[:tile, tile:rows] = theirs[tile:rows, :tile].T
                    break
                first, past = n * tile, (n + 1) * tile
                if past < order:
                    theirs[first:past, past:] = theirs[past:, first:past].T

        pl.when(jnp.logical_or(core == 1, last))(roots_arrived)

        @pl.when(jnp.logical_not(last))
        def _():
            left = roots[0, pl.ds(pl.multiple_of(core * rows, rows), rows), :]
            three[:rows] = jnp.dot(left, grad[j], preferred_element_type=f32).astype(bf16)
            pl.when(core == 0)(roots_arrived)
            staged[j] = (
                jnp.dot(three[:rows], roots[1], preferred_element_type=f32) * math.sqrt(order)
            ).astype(bf16)

        for n in range(PIECES + 1):
            root_part(n, core).wait_send()
        return carry

    lax.fori_loop(0, blocks, one_block, 0)
    for h in range(PIECES):
        for j in range(blocks):
            grad_remote(j, h).wait_send()
    for r in range(HALVES):
        for k in range(4):
            tok_remote(k, r).wait_send()
        for h in range(PIECES):
            for j in range(blocks):
                half(j, h, r, core).wait_send()
            for k in range(SENDS):
                hop(blocks - 1, k, h, r).wait_send()


def last_kernel(blocks, stats, roots, grad, staged, update, fresh, mixed, final, sems):
    f32, bf16 = jnp.float32, jnp.bfloat16
    order = grad.shape[1]
    rows = order // 2
    core = lax.rem(lax.axis_index("tok"), 2)
    copies = [
        pltpu.make_async_copy(stats.at[j], fresh.at[j, 0], sems.at[j]) for j in range(blocks)
    ]
    copies += [
        pltpu.make_async_copy(
            staged.at[j], update.at[:, j * order : (j + 1) * order], sems.at[blocks + j]
        )
        for j in range(blocks - 1)
    ]
    for copy in copies:
        copy.start()
    left = roots[0, pl.ds(pl.multiple_of(core * rows, rows), rows), :]
    mixed[...] = jnp.dot(left, grad[blocks - 1], preferred_element_type=f32).astype(bf16)
    for h in range(2):
        half = slice(h * (rows // 2), (h + 1) * (rows // 2))
        final[half] = (
            jnp.dot(mixed[half], roots[1], preferred_element_type=f32) * math.sqrt(order)
        ).astype(bf16)
        copy = pltpu.make_async_copy(
            final.at[half], update.at[half, (blocks - 1) * order :], sems.at[2 * blocks - 1 + h]
        )
        copy.start()
        copies.append(copy)
    for copy in copies:
        copy.wait()


def on_device(tokens, grads_out, statistics):
    blocks, _, order, piece_width = statistics.shape
    count = lax.axis_size("tok")
    if piece_width != order or count != 2 * LINE or tokens.shape[1] != LINE * order:
        return in_pieces(tokens, grads_out, statistics)
    local, rows, wide = tokens.shape[0], order // 2, order // PIECES
    part = rows // HALVES
    bf16, f32 = jnp.bfloat16, jnp.float32
    dma = pltpu.SemaphoreType.DMA
    anywhere = pl.BlockSpec(memory_space=pl.ANY)
    near = pl.BlockSpec(memory_space=pltpu.VMEM)
    square = pltpu.VMEM((order, order), bf16)
    held = pl.pallas_call(
        functools.partial(fused_kernel, blocks),
        out_shape=(
            pltpu.VMEM((blocks, order, order), f32),
            pltpu.VMEM((2, order, order), bf16),
            pltpu.VMEM((blocks, order, order), bf16),
            pltpu.VMEM((max(blocks - 1, 1), rows, order), bf16),
        ),
        in_specs=[anywhere] * 3,
        out_specs=(near,) * 4,
        scratch_shapes=[
            pltpu.VMEM((4, HALVES, 2 * local, part), bf16),
            pltpu.VMEM((blocks, PIECES, 2 * local, wide), bf16),
            pltpu.VMEM((SENDS, PIECES, HALVES, part, wide), bf16),
            pltpu.VMEM((blocks, SLOTS, PIECES, HALVES, part, wide), bf16),
            pltpu.VMEM((PIECES, HALVES, part, wide), f32),
            square,
            square,
            square,
            square,
            dma((4, HALVES)),
            dma((4, HALVES)),
            dma((4, HALVES)),
            dma((blocks, PIECES)),
            dma((blocks, PIECES)),
            dma((blocks, PIECES)),
            dma((SENDS, PIECES, HALVES)),
            dma((blocks, SLOTS, PIECES, HALVES)),
            dma((blocks, PIECES, HALVES)),
            dma((blocks, PIECES, HALVES)),
            dma((blocks,)),
            dma((PIECES + 1,)),
            dma((PIECES + 1,)),
        ],
        compiler_params=pltpu.CompilerParams(
            collective_id=0, has_side_effects=True, vmem_limit_bytes=46 << 20
        ),
    )(tokens, grads_out, statistics)
    return pl.pallas_call(
        functools.partial(last_kernel, blocks),
        out_shape=(
            jax.ShapeDtypeStruct((rows, blocks * order), bf16),
            jax.ShapeDtypeStruct(statistics.shape, f32),
        ),
        in_specs=[near] * 4,
        out_specs=(anywhere, anywhere),
        scratch_shapes=[
            pltpu.VMEM((rows, order), bf16),
            pltpu.VMEM((rows, order), bf16),
            dma((2 * blocks + 1,)),
        ],
        compiler_params=pltpu.CompilerParams(vmem_limit_bytes=24 << 20),
    )(*held)


def solution(mesh):
    placed = (P("tok", None), P("tok", "col"), P("col", "tok", None, None))
    return jax.shard_map(
        on_device,
        mesh=mesh,
        in_specs=placed,
        out_specs=(P("tok", "col"), P("col", "tok", None, None)),
        check_vma=False,
    )
```

```python
import functools
import math

import jax
import jax.numpy as jnp
from jax import lax
from jax.experimental import pallas as pl
from jax.experimental.pallas import tpu as pltpu
from jax.sharding import PartitionSpec as P

ITERS = 3


def swapped(block, axis, bit):
    count = lax.axis_size(axis)
    route = []
    for low in range(count):
        high = low | 1 << bit
        if high != low and high < count:
            route += [(low, high), (high, low)]
    return lax.ppermute(block, axis, route)


def as_sent(array):
    return jax.tree.map(lambda a: a.astype(jnp.bfloat16) if a.dtype == jnp.float32 else a, array)


def doubling(values, levels, device, axis_dim, partner):
    for level_bit in range(levels):
        partner_part = partner(values, level_bit)
        low_side = device // 2**level_bit % 2 == 0
        values = jnp.where(
            low_side,
            jnp.concatenate([values, partner_part], axis_dim),
            jnp.concatenate([partner_part, values], axis_dim),
        )
    return values


def product(left_side, right_side):
    return jnp.einsum("bij,bjk->bik", left_side, right_side, precision=lax.Precision.HIGHEST)


def in_pieces(tokens, grads_out, statistics):
    device = lax.axis_index("tok")
    blocks = statistics.shape[0]
    order_size = statistics.shape[2]
    piece_width = statistics.shape[3]
    pieces = order_size // piece_width
    levels = pieces.bit_length() - 1
    rows_dev = tokens.shape[1] // lax.axis_size("tok")
    side_bit = device // pieces % 2
    column = device % pieces
    slab_index = device % (2 * pieces)

    def columns_of(values):
        return lax.dynamic_slice_in_dim(values, column * piece_width, piece_width, 2)

    owned = lax.psum_scatter(
        lax.dot_general(
            tokens, grads_out, (((0,), (0,)), ((), ())), preferred_element_type=jnp.float32
        ),
        "tok",
        scatter_dimension=0,
        tiled=True,
    ).astype(jnp.bfloat16)
    gradient = doubling(
        owned, levels + 1, device, 0, lambda portion, level_bit: swapped(portion, "tok", level_bit)
    )
    grad_cube = gradient.reshape(order_size, blocks, order_size)
    forward = jnp.transpose(grad_cube, (1, 0, 2))
    backward = jnp.transpose(grad_cube, (1, 2, 0))
    oriented = jnp.where(side_bit == 0, forward, backward)
    own_rows = lax.dynamic_slice_in_dim(oriented, column * piece_width, piece_width, 1)
    gram_piece = jnp.einsum("brc,bqc->brq", oriented, own_rows, preferred_element_type=jnp.float32)
    fresh_stat = statistics[:, 0] + gram_piece
    identity = jnp.eye(order_size, dtype=jnp.float32)

    def widen(values):
        return doubling(
            values, levels, device, 2, lambda portion, level_bit: swapped(portion, "tok", level_bit)
        )

    assembled = widen(fresh_stat)
    scaling = (2.5 / jnp.sqrt(jnp.sum(assembled * assembled, axis=(1, 2)) + 1e-06))[:, None, None]
    matrix = scaling * assembled
    factor = (5.0 * identity - matrix) * 0.25
    iterate = jnp.sqrt(jnp.sqrt(scaling)) * columns_of(factor)
    for repeat in range(1, ITERS):
        square = widen(product(factor, columns_of(factor)))
        fourth = widen(product(square, columns_of(square)))
        matrix = widen(product(fourth, columns_of(matrix)))
        factor = (5.0 * identity - matrix) * 0.25
        iterate = product(factor, iterate)
    own_root = doubling(
        iterate.astype(jnp.bfloat16),
        levels,
        device,
        2,
        lambda portion, level_bit: jax.tree.map(
            lambda part, own: part.astype(own.dtype),
            swapped(as_sent(portion), "tok", level_bit),
            portion,
        ),
    )
    other_root = swapped(own_root, "tok", levels)
    left_root = jnp.where(side_bit == 0, own_root, other_root)
    right_root = jnp.where(side_bit == 0, other_root, own_root)
    left_rows = lax.dynamic_slice_in_dim(left_root, slab_index * rows_dev, rows_dev, 1)
    mixed_rows = jnp.einsum(
        "bsr,rbc->bsc", left_rows, grad_cube, preferred_element_type=jnp.float32
    ).astype(jnp.bfloat16)
    update = jnp.einsum(
        "bsc,bcd->sbd", mixed_rows, right_root, preferred_element_type=jnp.float32
    ) * math.sqrt(order_size)
    return (update.reshape(rows_dev, blocks * order_size).astype(jnp.bfloat16), fresh_stat[:, None])


LINE = 4
SENDS = 3
SLOTS = 5
PIECES = 4
HALVES = 2


def fused_kernel(
    blocks, tokens, grads, old, stats, roots, grad, staged,
    tok2, grad2, sent, got, own32, scaled, one, two, three,
    tok_in, tok_send, tok_recv, grad_in, grad_send, grad_recv, hop_send, hop_recv,
    half_send, half_recv, stat_in, root_send, root_recv,
):
    f32, bf16 = jnp.float32, jnp.bfloat16
    order = grad.shape[1]
    local = tokens.shape[0]
    rows = order // 2
    part_rows = rows // HALVES
    wide = tile = order // PIECES
    me = lax.axis_index("tok")
    spot, core = me // 2, lax.rem(me, 2)
    partner = spot * 2 + 1 - core
    outer = jnp.logical_or(spot == 0, spot == LINE - 1)
    inner = jnp.logical_not(outer)
    low = spot < LINE // 2
    near = spot + 1 - 2 * lax.rem(spot, 2)
    across = LINE - 1 - spot
    near_device, across_device = near * 2 + core, across * 2 + core

    def chunk_of(k):
        far = jnp.where(low, LINE - 1 - k, k)
        return jnp.where(k < 2, far, jnp.where(k == 2, near, spot))

    def remote(source, target, send, recv, device):
        return pltpu.make_async_remote_copy(
            src_ref=source, dst_ref=target, send_sem=send, recv_sem=recv,
            device_id={"tok": device}, device_id_type=pl.DeviceIdType.MESH,
        )

    def columns(k, r, owner):
        start = (chunk_of(k) * 2 + owner) * rows + r * part_rows
        return pl.ds(pl.multiple_of(start, part_rows), part_rows)

    def tok_local(k, r):
        return pltpu.make_async_copy(
            tokens.at[:, columns(k, r, core)], tok2.at[k, r, pl.ds(0, local), :], tok_in.at[k, r]
        )

    def tok_remote(k, r):
        return remote(
            tokens.at[:, columns(k, r, 1 - core)], tok2.at[k, r, pl.ds(local, local), :],
            tok_send.at[k, r], tok_recv.at[k, r], partner,
        )

    def grad_columns(j, h):
        return pl.ds(pl.multiple_of(j * order + h * wide, wide), wide)

    def grad_local(j, h):
        return pltpu.make_async_copy(
            grads.at[:, grad_columns(j, h)], grad2.at[j, h, pl.ds(0, local), :], grad_in.at[j, h]
        )

    def grad_remote(j, h):
        return remote(
            grads.at[:, grad_columns(j, h)], grad2.at[j, h, pl.ds(local, local), :],
            grad_send.at[j, h], grad_recv.at[j, h], partner,
        )

    def stat_load(j):
        return pltpu.make_async_copy(old.at[j, 0], stats.at[j], stat_in.at[j])

    def hop(j, k, h, r):
        slot = jnp.where(jnp.logical_or(outer, k == 2), k, SENDS + k)
        device = jnp.where(jnp.logical_or(outer, k == 2), near_device, across_device)
        return remote(
            sent.at[k, h, r], got.at[j, slot, h, r], hop_send.at[k, h, r],
            hop_recv.at[j, slot, h, r], device,
        )

    def arrived(j, slot, h, r):
        remote(
            sent.at[0, h, r], got.at[j, slot, h, r], hop_send.at[0, h, r],
            hop_recv.at[j, slot, h, r], near_device,
        ).wait_recv()

    def rows_of(owner, r):
        start = owner * rows + r * part_rows
        return pl.ds(pl.multiple_of(start, part_rows), part_rows)

    def half(j, h, r, owner):
        part = grad.at[j, rows_of(owner, r), pl.ds(h * wide, wide)]
        return remote(part, part, half_send.at[j, h, r], half_recv.at[j, h, r], partner)

    def root_part(n, side):
        if n == PIECES:
            part = roots.at[side, :rows, :tile]
        else:
            part = roots.at[side, n * tile if n else rows :, n * tile : (n + 1) * tile]
        return remote(part, part, root_send.at[n], root_recv.at[n], partner)

    barrier = pltpu.get_barrier_semaphore()
    pl.semaphore_signal(
        barrier, inc=1, device_id={"tok": partner}, device_id_type=pl.DeviceIdType.MESH
    )
    pl.semaphore_signal(
        barrier, inc=1, device_id={"tok": near_device}, device_id_type=pl.DeviceIdType.MESH
    )

    @pl.when(inner)
    def _():
        pl.semaphore_signal(
            barrier, inc=1, device_id={"tok": across_device}, device_id_type=pl.DeviceIdType.MESH
        )

    tok_local(0, 0).start()
    grad_local(0, 0).start()
    pl.semaphore_wait(barrier, jnp.where(inner, 3, 2))
    tok_remote(0, 0).start()
    grad_remote(0, 0).start()
    for r in range(1, HALVES):
        tok_local(0, r).start()
        tok_remote(0, r).start()
    for h in range(1, PIECES):
        grad_local(0, h).start()
        grad_remote(0, h).start()

    def partial(j, k, h, r, rows=slice(None)):
        return lax.dot_general(
            tok2[k, r, rows], grad2[j, h, rows], (((0,), (0,)), ((), ())),
            preferred_element_type=f32,
        )

    def piece(j, k, h):
        pl.when(k == 0)(lambda: grad_local(j, h).wait())
        if h:
            pl.when(k == 0)(lambda: grad_remote(j, h).wait_recv())
        for r in range(HALVES):
            if h == 0:
                pl.when(j == 0)(lambda: tok_local(k, r).wait())
                sent_part = partial(j, k, h, r, slice(0, local))
                if r == 0:
                    pl.when(k == 0)(lambda: grad_remote(j, h).wait_recv())
                pl.when(j == 0)(lambda: tok_remote(k, r).wait_recv())
                sent_part = sent_part + partial(j, k, h, r, slice(local, 2 * local))
            else:
                sent_part = partial(j, k, h, r)

            @pl.when(j > 0)
            def _():
                hop(j - 1, k, h, r).wait_send()

            @pl.when(outer)
            def _():
                sent[k, h, r] = sent_part.astype(bf16)

            @pl.when(inner)
            def _():
                slot = jnp.where(k == 2, SENDS, k)
                arrived(j, slot, h, r)
                sent[k, h, r] = (sent_part + got[j, slot, h, r].astype(f32)).astype(bf16)

            hop(j, k, h, r).start()

    def step(s, carry):
        j, r = s // SENDS, lax.rem(s, SENDS)
        k = jnp.where(outer, r, lax.rem(SENDS - r, SENDS))

        for h in range(PIECES):
            piece(j, k, h)

        @pl.when(s == 0)
        def _():
            for later in range(1, 4):
                for r in range(HALVES):
                    tok_local(later, r).start()
                    tok_remote(later, r).start()

        @pl.when(s == 1)
        def _():
            for later in range(1, blocks):
                for h in range(PIECES):
                    grad_local(later, h).start()
                    grad_remote(later, h).start()
            for later in range(blocks):
                stat_load(later).start()

        return carry

    def put(ref, n, value):
        value = value.astype(bf16)
        ref[n : n + tile, n:] = value
        if n + tile < order:
            ref[n + tile :, n : n + tile] = value[:, tile:].T

    def product(left, right, finish, step=1, first=0):
        for n in range(first * tile, order, tile)[::step]:
            total = jnp.dot(left[n : n + tile, :], right[:, n:], preferred_element_type=f32)
            finish(total, n, (slice(n, n + tile), slice(n, None)))

    def one_block(j, carry):
        stat = stats.at[j]
        last = j == blocks - 1
        split = blocks * SENDS
        first = jnp.where(outer, jnp.where(j == 0, 0, split), j * SENDS + jnp.minimum(j, 1))
        end = jnp.where(outer, split, (j + 1) * SENDS)
        lax.fori_loop(first, end, step, 0)

        @pl.when(j == 0)
        def _():
            for r in range(HALVES):
                tok_local(SENDS, r).wait()
                tok_remote(SENDS, r).wait_recv()

        def ahead(h):
            @pl.when(jnp.logical_and(inner, jnp.logical_not(last)))
            def _():
                piece(j + 1, 0, h)

        for h in range(PIECES):
            for r in range(HALVES):
                own32[h, r] = partial(j, SENDS, h, r)

        @pl.when(inner)
        def _():
            for h in range(PIECES):
                for r in range(HALVES):
                    arrived(j, SENDS + 1, h, r)
                    own32[h, r] = own32[h, r] + got[j, SENDS + 1, h, r].astype(f32)

        stat_load(j).wait()

        def norm(total, own, other):
            square = jnp.sum(total * total, axis=0, keepdims=True)
            value = jnp.sum(square[:, own], axis=1, keepdims=True)
            if other is not None:
                value = value + 2.0 * jnp.sum(square[:, other], axis=1, keepdims=True)
            return value

        def gram_left(h):
            columns = slice(h * wide, (h + 1) * wide)
            sums = jnp.zeros((1, 1), f32)
            for n in range(0, order, tile):
                at = (slice(n, n + tile), slice(n, None))
                total = stat[at] + lax.dot_general(
                    grad[j, n : n + tile, columns], grad[j, n:, columns],
                    (((1,), (1,)), ((), ())), preferred_element_type=f32,
                )
                stat[at] = total
                if h == PIECES - 1:
                    put(scaled, n, total)
                    rest = slice(tile, None) if n + tile < order else None
                    sums = sums + norm(total, slice(0, tile), rest)
            if h == PIECES - 1:
                own32[0, 0, 0:1, 0:wide] = jnp.broadcast_to(sums, (1, wide))

        def gram_right(h):
            n, reach = h * tile, (h + 1) * tile
            total = stat[:reach, n:reach] + lax.dot_general(
                grad[j, :, :reach], grad[j, :, n:reach], (((0,), (0,)), ((), ())),
                preferred_element_type=f32,
            )
            stat[:reach, n:reach] = total
            scaled[:reach, n:reach] = total.astype(bf16)
            diagonal = total[n:]
            sums = jnp.sum(jnp.sum(diagonal * diagonal, axis=0, keepdims=True), axis=1, keepdims=True)
            if h:
                above = total[:n]
                scaled[n:reach, :n] = above.astype(bf16).T
                sums = sums + 2.0 * jnp.sum(
                    jnp.sum(above * above, axis=0, keepdims=True), axis=1, keepdims=True
                )
                sums = sums + own32[0, 0, 0:1, 0:1]
            own32[0, 0, 0:1, 0:wide] = jnp.broadcast_to(sums, (1, wide))

        for h in range(PIECES):
            for r in range(HALVES):
                arrived(j, 2, h, r)

                total = own32[h, r] + got[j, 2, h, r].astype(f32)
                grad[j, rows_of(core, r), h * wide : (h + 1) * wide] = total.astype(bf16)
                half(j, h, r, core).start()
            for r in range(HALVES):
                half(j, h, r, 1 - core).wait_recv()
            pl.when(core == 0)(functools.partial(gram_left, h))
            pl.when(core == 1)(functools.partial(gram_right, h))

        zeta = 2.5 / jnp.sqrt(own32[0, 0, 0:1, 0:1] + 1e-06)
        gain = jnp.sqrt(jnp.sqrt(zeta))

        def lower_half(n):
            if n + tile < order:
                stat[n + tile :, n : n + tile] = stat[n : n + tile, n + tile :].T

        def first_square(total, n, at):
            put(one, n, (zeta * zeta * 0.0625) * total - (0.625 * zeta) * stat[at])
            if n:
                lower_half(n)

        product(scaled, scaled, first_square)

        def first_fourth(total, n, at):
            put(two, n, 3.125 * one[at].astype(f32) + total)
            if n == 0:
                lower_half(n)

        product(one, one, first_fourth)

        def second(total, n, at):
            put(three, n, zeta * (2.44140625 * stat[at] + total))

        product(two, scaled, second)

        def second_square(total, n, at):
            base = three[at].astype(f32)
            put(one, n, (total - 10.0 * base) * 0.0625)
            put(two, n, (5.0 * base - total) * 0.25)

        product(three, three, second_square)
        mine = roots.at[core]

        def second_fourth(total, n, at):
            put(mine, n, 3.125 * one[at].astype(f32) + total)

        product(one, one, second_fourth)
        ahead(0)
        ahead(1)

        def factors(total, n, at):
            value = -0.25 * (
                1.25 * three[at].astype(f32) + 2.44140625 * two[at].astype(f32) + total
            )
            put(one, n, value)

        product(mine, two, factors)

        def final(total, n, at):
            shape = total.shape
            unit = (
                lax.broadcasted_iota(jnp.int32, shape, 0) + n
                == lax.broadcasted_iota(jnp.int32, shape, 1) + at[1].start
            ).astype(f32)
            rest = one[at].astype(f32)
            value = 1.953125 * unit + 1.25 * rest - zeta * (0.390625 * stat[at] + 0.25 * total)
            return gain * value

        def final_rows(total, n, at):
            put(mine, n, final(total, n, at))
            root_part(n // tile, core).start()

        def final_first(start, end):
            at = (slice(0, tile), slice(start, end))
            total = jnp.dot(one[:tile, :], scaled[:, start:end], preferred_element_type=f32)
            value = final(total, 0, at).astype(bf16)
            mine[at] = value
            skip = 0 if start else tile
            mine[start + skip : end, :tile] = value[:, skip:].T

        product(one, scaled, final_rows, -1, 1)
        final_first(rows, order)
        root_part(0, core).start()
        final_first(0, rows)
        root_part(PIECES, core).start()
        ahead(2)
        ahead(3)

        def roots_arrived():
            theirs = roots.at[1 - core]
            for n in range(PIECES)[::-1]:
                root_part(n, 1 - core).wait_recv()
                if n == 0:
                    theirs[:tile, rows:] = theirs[rows:, :tile].T
                    root_part(PIECES, 1 - core).wait_recv()
                    theirs[:tile, tile:rows] = theirs[tile:rows, :tile].T
                    break
                first, past = n * tile, (n + 1) * tile
                if past < order:
                    theirs[first:past, past:] = theirs[past:, first:past].T

        pl.when(jnp.logical_or(core == 1, last))(roots_arrived)

        @pl.when(jnp.logical_not(last))
        def _():
            left = roots[0, pl.ds(pl.multiple_of(core * rows, rows), rows), :]
            three[:rows] = jnp.dot(left, grad[j], preferred_element_type=f32).astype(bf16)
            pl.when(core == 0)(roots_arrived)
            staged[j] = (
                jnp.dot(three[:rows], roots[1], preferred_element_type=f32) * math.sqrt(order)
            ).astype(bf16)

        for n in range(PIECES + 1):
            root_part(n, core).wait_send()
        return carry

    lax.fori_loop(0, blocks, one_block, 0)
    for h in range(PIECES):
        for j in range(blocks):
            grad_remote(j, h).wait_send()
    for r in range(HALVES):
        for k in range(4):
            tok_remote(k, r).wait_send()
        for h in range(PIECES):
            for j in range(blocks):
                half(j, h, r, core).wait_send()
            for k in range(SENDS):
                hop(blocks - 1, k, h, r).wait_send()


def last_kernel(blocks, stats, roots, grad, staged, update, fresh, mixed, final, sems):
    f32, bf16 = jnp.float32, jnp.bfloat16
    order = grad.shape[1]
    rows = order // 2
    core = lax.rem(lax.axis_index("tok"), 2)
    copies = [
        pltpu.make_async_copy(stats.at[j], fresh.at[j, 0], sems.at[j]) for j in range(blocks)
    ]
    copies += [
        pltpu.make_async_copy(
            staged.at[j], update.at[:, j * order : (j + 1) * order], sems.at[blocks + j]
        )
        for j in range(blocks - 1)
    ]
    for copy in copies:
        copy.start()
    left = roots[0, pl.ds(pl.multiple_of(core * rows, rows), rows), :]
    mixed[...] = jnp.dot(left, grad[blocks - 1], preferred_element_type=f32).astype(bf16)
    for h in range(2):
        half = slice(h * (rows // 2), (h + 1) * (rows // 2))
        final[half] = (
            jnp.dot(mixed[half], roots[1], preferred_element_type=f32) * math.sqrt(order)
        ).astype(bf16)
        copy = pltpu.make_async_copy(
            final.at[half], update.at[half, (blocks - 1) * order :], sems.at[2 * blocks - 1 + h]
        )
        copy.start()
        copies.append(copy)
    for copy in copies:
        copy.wait()


def on_device(tokens, grads_out, statistics):
    blocks, _, order, piece_width = statistics.shape
    count = lax.axis_size("tok")
    if piece_width != order or count != 2 * LINE or tokens.shape[1] != LINE * order:
        return in_pieces(tokens, grads_out, statistics)
    local, rows, wide = tokens.shape[0], order // 2, order // PIECES
    part = rows // HALVES
    bf16, f32 = jnp.bfloat16, jnp.float32
    dma = pltpu.SemaphoreType.DMA
    anywhere = pl.BlockSpec(memory_space=pl.ANY)
    near = pl.BlockSpec(memory_space=pltpu.VMEM)
    square = pltpu.VMEM((order, order), bf16)
    held = pl.pallas_call(
        functools.partial(fused_kernel, blocks),
        out_shape=(
            pltpu.VMEM((blocks, order, order), f32),
            pltpu.VMEM((2, order, order), bf16),
            pltpu.VMEM((blocks, order, order), bf16),
            pltpu.VMEM((max(blocks - 1, 1), rows, order), bf16),
        ),
        in_specs=[anywhere] * 3,
        out_specs=(near,) * 4,
        scratch_shapes=[
            pltpu.VMEM((4, HALVES, 2 * local, part), bf16),
            pltpu.VMEM((blocks, PIECES, 2 * local, wide), bf16),
            pltpu.VMEM((SENDS, PIECES, HALVES, part, wide), bf16),
            pltpu.VMEM((blocks, SLOTS, PIECES, HALVES, part, wide), bf16),
            pltpu.VMEM((PIECES, HALVES, part, wide), f32),
            square,
            square,
            square,
            square,
            dma((4, HALVES)),
            dma((4, HALVES)),
            dma((4, HALVES)),
            dma((blocks, PIECES)),
            dma((blocks, PIECES)),
            dma((blocks, PIECES)),
            dma((SENDS, PIECES, HALVES)),
            dma((blocks, SLOTS, PIECES, HALVES)),
            dma((blocks, PIECES, HALVES)),
            dma((blocks, PIECES, HALVES)),
            dma((blocks,)),
            dma((PIECES + 1,)),
            dma((PIECES + 1,)),
        ],
        compiler_params=pltpu.CompilerParams(
            collective_id=0, has_side_effects=True, vmem_limit_bytes=46 << 20
        ),
    )(tokens, grads_out, statistics)
    return pl.pallas_call(
        functools.partial(last_kernel, blocks),
        out_shape=(
            jax.ShapeDtypeStruct((rows, blocks * order), bf16),
            jax.ShapeDtypeStruct(statistics.shape, f32),
        ),
        in_specs=[near] * 4,
        out_specs=(anywhere, anywhere),
        scratch_shapes=[
            pltpu.VMEM((rows, order), bf16),
            pltpu.VMEM((rows, order), bf16),
            dma((2 * blocks + 1,)),
        ],
        compiler_params=pltpu.CompilerParams(vmem_limit_bytes=24 << 20),
    )(*held)


def solution(mesh):
    placed = (P("tok", None), P("tok", "col"), P("col", "tok", None, None))
    return jax.shard_map(
        on_device,
        mesh=mesh,
        in_specs=placed,
        out_specs=(P("tok", "col"), P("col", "tok", None, None)),
        check_vma=False,
    )
```
